8 devices in a mesh: dp: 1 (over z), tp: 2 (over y), sp: 4 (over x, core).
Axes of the slice: x: 2, y: 2, z: 1, core: 2. Of those that a mesh axis runs over, the one named last changes fastest.
Arguments:
- tok_emb: bfloat16 [4, 32, 4096], P(None, 'dp')
- lengths: int32 [32], P('dp')
- key_cache: bfloat16 [2, 32, 1024, 8, 128], P(None, 'dp', 'sp', 'tp')
- val_cache: bfloat16 [2, 32, 1024, 8, 128], P(None, 'dp', 'sp', 'tp')
- gain_attn: bfloat16 [2, 4096], replicated
- gain_mlp: bfloat16 [2, 4096], replicated
- w_query: bfloat16 [2, 4096, 4096], P(None, None, 'tp')
- w_key: bfloat16 [2, 4096, 1024], P(None, None, 'tp')
- w_value: bfloat16 [2, 4096, 1024], P(None, None, 'tp')
- w_out: bfloat16 [2, 4096, 4096], P(None, 'tp')
- w_gate: bfloat16 [2, 4096, 14336], P(None, None, 'tp')
- w_up: bfloat16 [2, 4096, 14336], P(None, None, 'tp')
- w_down: bfloat16 [2, 14336, 4096], P(None, 'tp')
Outputs:
- output 1: bfloat16 [4, 32, 4096], P(None, 'dp')
- output 2: bfloat16 [2, 32, 1024, 8, 128], P(None, 'dp', 'sp', 'tp')
- output 3: bfloat16 [2, 32, 1024, 8, 128], P(None, 'dp', 'sp', 'tp')
All inputs are finite; a program needn't handle non-finite values.
Results may differ from the reference program's by a relative error of at most 0.0144379.
Values sent between devices are 32-bit elements.
A program may use at most 2 GiB of HBM per device.

```python
import math
import jax
import jax.numpy as jnp
from jax import lax

N_STEPS = 4
N_LAYERS = 2
SEQ_BATCH = 32
LOC_LEN = 256
SP_SIZE = 4
D_MODEL = 4096
N_HEADS = 32
KV_HEADS = 8
HEAD_DIM = 128
FF_DIM = 14336
CACHE_LEN = LOC_LEN * SP_SIZE
GROUP_SIZE = N_HEADS // KV_HEADS
EPS = 1e-5
ROPE_BASE = 500000.0


def draw_lengths(len_key, perm_key):
    drawn_len = jax.random.randint(len_key, (SEQ_BATCH,), CACHE_LEN // 2, CACHE_LEN - N_STEPS + 1)
    perm_ids = jax.random.permutation(perm_key, SEQ_BATCH)
    lengths = jnp.where(perm_ids == 0, CACHE_LEN - N_STEPS, jnp.where(perm_ids == 1, CACHE_LEN // 2, drawn_len))
    return lengths.astype(jnp.int32)


def draw_scales():
    score_var = max(math.log(CACHE_LEN / 32.0), 1.0)
    plant_gain = (math.log(CACHE_LEN) + 0.5 * score_var) / math.sqrt(HEAD_DIM)
    key_scale = math.sqrt(score_var / (1.0 + plant_gain * plant_gain))
    return plant_gain, key_scale


def setup_inputs(seed: int = 0, part: int = 0) -> dict:
    plant_gain, key_scale = draw_scales()
    part_keys = jax.random.split(jax.random.fold_in(jax.random.key(seed), part), 6)
    weight_keys = jax.random.split(jax.random.key(seed + 1), 9)
    common = jax.random.normal(part_keys[0], (SEQ_BATCH, D_MODEL), jnp.float32)
    step_noise = jax.random.normal(part_keys[1], (N_STEPS, SEQ_BATCH, D_MODEL), jnp.float32)
    tok_emb = ((common[None] + 0.4 * step_noise) / math.sqrt(1.16)).astype(jnp.bfloat16)
    lengths = draw_lengths(part_keys[2], part_keys[3])
    cache_shape = (N_LAYERS, SEQ_BATCH, CACHE_LEN, KV_HEADS, HEAD_DIM)
    key_cache = (key_scale * jax.random.normal(part_keys[4], cache_shape, jnp.float32)).astype(jnp.bfloat16)
    val_cache = jax.random.normal(part_keys[5], cache_shape, jnp.float32).astype(jnp.bfloat16)
    gain_attn = (1.0 + 0.3 * jax.random.normal(weight_keys[0], (N_LAYERS, D_MODEL), jnp.float32)).astype(jnp.bfloat16)
    gain_mlp = (1.0 + 0.3 * jax.random.normal(weight_keys[1], (N_LAYERS, D_MODEL), jnp.float32)).astype(jnp.bfloat16)
    in_scale = D_MODEL ** -0.5
    key_proj = jax.random.normal(weight_keys[2], (N_LAYERS, D_MODEL, KV_HEADS, HEAD_DIM), jnp.float32) * in_scale
    query_proj = plant_gain * jnp.repeat(key_proj, GROUP_SIZE, axis=2) + jax.random.normal(weight_keys[3], (N_LAYERS, D_MODEL, N_HEADS, HEAD_DIM), jnp.float32) * in_scale
    w_query = query_proj.reshape(N_LAYERS, D_MODEL, N_HEADS * HEAD_DIM).astype(jnp.bfloat16)
    w_key = key_proj.reshape(N_LAYERS, D_MODEL, KV_HEADS * HEAD_DIM).astype(jnp.bfloat16)
    w_value = (jax.random.normal(weight_keys[4], (N_LAYERS, D_MODEL, KV_HEADS * HEAD_DIM), jnp.float32) * in_scale).astype(jnp.bfloat16)
    w_out = (jax.random.normal(weight_keys[5], (N_LAYERS, N_HEADS * HEAD_DIM, D_MODEL), jnp.float32) * (N_HEADS * HEAD_DIM) ** -0.5).astype(jnp.bfloat16)
    w_gate = (jax.random.normal(weight_keys[6], (N_LAYERS, D_MODEL, FF_DIM), jnp.float32) * in_scale).astype(jnp.bfloat16)
    w_up = (jax.random.normal(weight_keys[7], (N_LAYERS, D_MODEL, FF_DIM), jnp.float32) * in_scale).astype(jnp.bfloat16)
    w_down = (jax.random.normal(weight_keys[8], (N_LAYERS, FF_DIM, D_MODEL), jnp.float32) * FF_DIM ** -0.5).astype(jnp.bfloat16)
    return {'tok_emb': tok_emb, 'lengths': lengths, 'key_cache': key_cache, 'val_cache': val_cache, 'gain_attn': gain_attn, 'gain_mlp': gain_mlp, 'w_query': w_query, 'w_key': w_key, 'w_value': w_value, 'w_out': w_out, 'w_gate': w_gate, 'w_up': w_up, 'w_down': w_down}


def rms_norm(hidden, gain_vec):
    x_float = hidden.astype(jnp.float32)
    inv_rms = lax.rsqrt(jnp.mean(x_float * x_float, axis=-1, keepdims=True) + EPS)
    return (x_float * inv_rms * gain_vec.astype(jnp.float32)).astype(jnp.bfloat16)


def rotary(in_vecs, positions):
    head_dim = in_vecs.shape[-1]
    half_dim = head_dim // 2
    inv_freq = 1.0 / (ROPE_BASE ** (jnp.arange(half_dim).astype(jnp.float32) * 2.0 / head_dim))
    angles = positions.astype(jnp.float32)[:, None] * inv_freq[None, :]
    cos_a = jnp.cos(angles)[:, None, :]
    sin_a = jnp.sin(angles)[:, None, :]
    front_half = in_vecs[..., :half_dim]
    back_half = in_vecs[..., half_dim:]
    return jnp.concatenate([front_half * cos_a - back_half * sin_a, back_half * cos_a + front_half * sin_a], axis=-1)


def reference(tok_emb, lengths, key_cache, val_cache, gain_attn, gain_mlp, w_query, w_key, w_value, w_out, w_gate, w_up, w_down):
    slot_ids = jnp.arange(CACHE_LEN)
    slot_pos = (slot_ids % LOC_LEN) * SP_SIZE + slot_ids // LOC_LEN
    row_ids = jnp.arange(SEQ_BATCH)

    def one_step(caches, step_in):
        step_idx, hidden = step_in
        cur_pos = lengths + step_idx
        write_slot = (cur_pos % SP_SIZE) * LOC_LEN + cur_pos // SP_SIZE
        valid_mask = (slot_pos[None, :] <= cur_pos[:, None])[:, None, None, :]

        def one_layer(hidden, layer_in):
            lay_k, lay_v, gain_a, gain_m, lay_wq, lay_wk, lay_wv, lay_wo, lay_wg, lay_wu, lay_wd = layer_in
            normed = rms_norm(hidden, gain_a)
            q_vec = jnp.dot(normed, lay_wq, preferred_element_type=jnp.float32).reshape(SEQ_BATCH, N_HEADS, HEAD_DIM)
            k_vec = jnp.dot(normed, lay_wk, preferred_element_type=jnp.float32).reshape(SEQ_BATCH, KV_HEADS, HEAD_DIM)
            v_vec = jnp.dot(normed, lay_wv, preferred_element_type=jnp.float32).reshape(SEQ_BATCH, KV_HEADS, HEAD_DIM).astype(jnp.bfloat16)
            q_rot = rotary(q_vec, cur_pos).astype(jnp.bfloat16).reshape(SEQ_BATCH, KV_HEADS, GROUP_SIZE, HEAD_DIM)
            k_rot = rotary(k_vec, cur_pos).astype(jnp.bfloat16)
            lay_k = lay_k.at[row_ids, write_slot].set(k_rot)
            lay_v = lay_v.at[row_ids, write_slot].set(v_vec)
            scores = jnp.einsum('bkgd,bjkd->bkgj', q_rot.astype(jnp.float32), lay_k.astype(jnp.float32)) * HEAD_DIM ** -0.5
            scores = jnp.where(valid_mask, scores, -1e30)
            prob_w = jnp.exp(scores - jnp.max(scores, axis=-1, keepdims=True))
            denom_sum = jnp.sum(prob_w, axis=-1, keepdims=True)
            numer_sum = jnp.einsum('bkgj,bjkd->bkgd', prob_w.astype(jnp.bfloat16).astype(jnp.float32), lay_v.astype(jnp.float32))
            attn_out = (numer_sum / denom_sum).astype(jnp.bfloat16).reshape(SEQ_BATCH, N_HEADS * HEAD_DIM)
            hidden = (hidden.astype(jnp.float32) + jnp.dot(attn_out, lay_wo, preferred_element_type=jnp.float32)).astype(jnp.bfloat16)
            normed = rms_norm(hidden, gain_m)
            gate_pre = jnp.dot(normed, lay_wg, preferred_element_type=jnp.float32)
            up_pre = jnp.dot(normed, lay_wu, preferred_element_type=jnp.float32)
            mlp_act = (jax.nn.silu(gate_pre) * up_pre).astype(jnp.bfloat16)
            hidden = (hidden.astype(jnp.float32) + jnp.dot(mlp_act, lay_wd, preferred_element_type=jnp.float32)).astype(jnp.bfloat16)
            return hidden, (lay_k, lay_v)

        hidden, new_caches = lax.scan(one_layer, hidden, (caches[0], caches[1], gain_attn, gain_mlp, w_query, w_key, w_value, w_out, w_gate, w_up, w_down))
        return new_caches, hidden

    final_caches, hidden_all = lax.scan(one_step, (key_cache, val_cache), (jnp.arange(N_STEPS), tok_emb))
    return (hidden_all, final_caches[0], final_caches[1])
```

```python
import jax
import jax.numpy as jnp
from jax import lax
from jax.sharding import PartitionSpec as P

EPS = 1e-5
ROPE_BASE = 500000.0


def rms_norm(hidden, gain_vec):
    x_float = hidden.astype(jnp.float32)
    inv_rms = lax.rsqrt(jnp.mean(x_float * x_float, axis=-1, keepdims=True) + EPS)
    return (x_float * inv_rms * gain_vec.astype(jnp.float32)).astype(jnp.bfloat16)


def rope_tables(positions, head_dim):
    half_dim = head_dim // 2
    inv_freq = 1.0 / (ROPE_BASE ** (jnp.arange(half_dim).astype(jnp.float32) * 2.0 / head_dim))
    angles = positions.astype(jnp.float32)[:, None] * inv_freq[None, :]
    return jnp.cos(angles)[:, None, :], jnp.sin(angles)[:, None, :]


def rotary(in_vecs, cos_a, sin_a):
    half_dim = in_vecs.shape[-1] // 2
    front = in_vecs[..., :half_dim]
    back = in_vecs[..., half_dim:]
    return jnp.concatenate([front * cos_a - back * sin_a, back * cos_a + front * sin_a], axis=-1)


def project(normed, weight):
    return jnp.dot(normed, weight, preferred_element_type=jnp.float32)


def solution(mesh):
    sp_size = mesh.shape['sp']

    def local_fn(tok_emb, lengths, key_cache, val_cache, gain_attn, gain_mlp, w_query, w_key, w_value, w_out, w_gate, w_up, w_down):
        n_steps, n_batch, d_model = tok_emb.shape
        n_layers, _, loc_len, kv_loc, head_dim = key_cache.shape
        heads_loc = w_query.shape[2] // head_dim
        group = heads_loc // kv_loc
        rows = n_steps * n_batch
        my_sp = lax.axis_index('sp')
        slot_pos = jnp.arange(loc_len) * sp_size + my_sp
        row_ids = jnp.arange(n_batch)
        cur_pos = lengths[None, :] + jnp.arange(n_steps)[:, None]
        write_slot = jnp.where(cur_pos % sp_size == my_sp, cur_pos // sp_size, loc_len)
        valid = (slot_pos[None, None, :] <= cur_pos[:, :, None])
        valid = valid.transpose(1, 0, 2)[:, None, :, None, :]
        cos_a, sin_a = rope_tables(cur_pos.reshape(rows), head_dim)
        hidden = tok_emb.reshape(rows, d_model)
        new_keys, new_vals = key_cache, val_cache
        for layer in range(n_layers):
            normed = rms_norm(hidden, gain_attn[layer])
            q_vec = project(normed, w_query[layer]).reshape(rows, heads_loc, head_dim)
            k_vec = project(normed, w_key[layer]).reshape(rows, kv_loc, head_dim)
            v_vec = project(normed, w_value[layer]).reshape(n_steps, n_batch, kv_loc, head_dim).astype(jnp.bfloat16)
            q_rot = rotary(q_vec, cos_a, sin_a).astype(jnp.bfloat16).reshape(n_steps, n_batch, kv_loc, group, head_dim)
            k_rot = rotary(k_vec, cos_a, sin_a).astype(jnp.bfloat16).reshape(n_steps, n_batch, kv_loc, head_dim)
            for s in range(n_steps):
                new_keys = new_keys.at[layer, row_ids, write_slot[s]].set(k_rot[s], mode='drop')
                new_vals = new_vals.at[layer, row_ids, write_slot[s]].set(v_vec[s], mode='drop')
            scores = jnp.einsum('sbkgd,bjkd->bksgj', q_rot, new_keys[layer], preferred_element_type=jnp.float32) * head_dim ** -0.5
            scores = jnp.where(valid, scores, -1e30)
            loc_max = jnp.max(scores, axis=-1, keepdims=True)
            prob_w = jnp.exp(scores - loc_max)
            loc_sum = jnp.sum(prob_w, axis=-1, keepdims=True)
            loc_out = jnp.einsum('bksgj,bjkd->bksgd', prob_w.astype(jnp.bfloat16), new_vals[layer], preferred_element_type=jnp.float32)
            glob_max = lax.pmax(loc_max, 'sp')
            merged = lax.psum(jnp.concatenate([loc_out, loc_sum], axis=-1) * jnp.exp(loc_max - glob_max), 'sp')
            attn_out = (merged[..., :head_dim] / merged[..., head_dim:]).astype(jnp.bfloat16)
            attn_out = attn_out.transpose(2, 0, 1, 3, 4).reshape(rows, heads_loc * head_dim)
            proj_sum = lax.psum(project(attn_out, w_out[layer]), 'tp')
            hidden = (hidden.astype(jnp.float32) + proj_sum).astype(jnp.bfloat16)
            normed = rms_norm(hidden, gain_mlp[layer])
            mlp_act = (jax.nn.silu(project(normed, w_gate[layer])) * project(normed, w_up[layer])).astype(jnp.bfloat16)
            down_sum = lax.psum(project(mlp_act, w_down[layer]), 'tp')
            hidden = (hidden.astype(jnp.float32) + down_sum).astype(jnp.bfloat16)
        return hidden.reshape(n_steps, n_batch, d_model), new_keys, new_vals

    cache_spec = P(None, 'dp', 'sp', 'tp', None)
    col_spec = P(None, None, 'tp')
    row_spec = P(None, 'tp', None)
    emb_spec = P(None, 'dp', None)
    return jax.shard_map(local_fn, mesh=mesh, in_specs=(emb_spec, P('dp'), cache_spec, cache_spec, P(), P(), col_spec, col_spec, col_spec, row_spec, col_spec, col_spec, row_spec), out_specs=(emb_spec, cache_spec, cache_spec), check_vma=False)
```

```python
import functools

import jax
import jax.numpy as jnp
from jax import lax
from jax.experimental import pallas as pl
from jax.experimental.pallas import tpu as pltpu
from jax.sharding import PartitionSpec as P

EPS = 1e-5
ROPE_BASE = 500000.0
F32 = jnp.float32
BF16 = jnp.bfloat16
MESH = pl.DeviceIdType.MESH
PC = 256
LOG2E = 1.4426950408889634


def rope_tables(positions, head_dim):
    half_dim = head_dim // 2
    inv_freq = 1.0 / (ROPE_BASE ** (jnp.arange(half_dim).astype(F32) * 2.0 / head_dim))
    angles = positions.astype(F32)[:, None] * inv_freq[None, :]
    cos_a, sin_a = jnp.cos(angles), jnp.sin(angles)
    return jnp.concatenate([cos_a, cos_a], -1), jnp.concatenate([-sin_a, sin_a], -1)


def qkv_kernel(u_ref, gain_ref, cos_ref, sin_ref, wq_ref, wk_ref, wv_ref, q_ref, k_ref, v_ref, h_scr):
    hd = cos_ref.shape[1]
    d_model = u_ref.shape[1]

    @pl.when(pl.program_id(0) == 0)
    def _():
        x = u_ref[...].astype(F32)
        inv = lax.rsqrt(jnp.sum(x * x, axis=-1, keepdims=True) * (1.0 / d_model) + EPS)
        h_scr[...] = (x * inv * gain_ref[...].astype(F32)).astype(BF16)

    h = h_scr[...]
    cos_a, sin_a = cos_ref[...], sin_ref[...]

    def rot(x):
        return (x * cos_a + pltpu.roll(x, hd // 2, 1) * sin_a).astype(BF16)

    q = jnp.dot(h, wq_ref[0], preferred_element_type=F32)
    for j in range(q_ref.shape[0]):
        q_ref[j] = rot(q[:, j * hd:(j + 1) * hd]).astype(F32)
    k = jnp.dot(h, wk_ref[0], preferred_element_type=F32)
    k_ref[0] = rot(k)
    v = jnp.dot(h, wv_ref[0], preferred_element_type=F32)
    v_ref[0] = v.astype(BF16)


def qkv_call(layer, u, gain, cos_a, sin_a, wq, wk, wv, hd):
    rows, d_model = u.shape
    kv_loc = wk.shape[2] // hd
    heads = wq.shape[2] // hd
    grp = heads // kv_loc
    full = lambda shape: pl.BlockSpec(shape, lambda j: (0,) * len(shape))
    return pl.pallas_call(
        qkv_kernel,
        grid=(kv_loc,),
        in_specs=[
            full((rows, d_model)), full((1, d_model)), full((rows, hd)), full((rows, hd)),
            pl.BlockSpec((1, d_model, grp * hd), lambda j: (layer, 0, j)),
            pl.BlockSpec((1, d_model, hd), lambda j: (layer, 0, j)),
            pl.BlockSpec((1, d_model, hd), lambda j: (layer, 0, j)),
        ],
        out_specs=[
            pl.BlockSpec((grp, rows, hd), lambda j: (j, 0, 0)),
            pl.BlockSpec((1, rows, hd), lambda j: (j, 0, 0)),
            pl.BlockSpec((1, rows, hd), lambda j: (j, 0, 0)),
        ],
        out_shape=[
            jax.ShapeDtypeStruct((heads, rows, hd), F32),
            jax.ShapeDtypeStruct((kv_loc, rows, hd), BF16),
            jax.ShapeDtypeStruct((kv_loc, rows, hd), BF16),
        ],
        scratch_shapes=[pltpu.VMEM((rows, d_model), BF16)],
        compiler_params=pltpu.CompilerParams(vmem_limit_bytes=60 * 2**20),
        name=f'qkv{layer}',
    )(u, gain, cos_a, sin_a, wq, wk, wv)


def attn_kernel(n_kv, n_steps, sp_size, has_prev, meta, q_ref, kn_ref, vn_ref, k_ref, v_ref, *rest):
    if has_prev:
        rest = rest[2:]
    ko_ref, vo_ref, o_ref, sm_ref, sl_ref, code = rest
    pair = pl.program_id(0)
    n_batch = pl.num_programs(0) * 2
    my_sp = meta[n_batch]
    heads, r8, hd = q_ref.shape
    rows = heads * r8
    n_cols = k_ref.shape[2]
    row_kv = rows // n_kv

    @pl.when(pair == 0)
    def _():
        ri = lax.broadcasted_iota(jnp.int32, (rows, n_cols), 0)
        ci = lax.broadcasted_iota(jnp.int32, (rows, n_cols), 1)
        same = (ci % n_kv) == (ri // row_kv)
        code[...] = jnp.where(same, (ci // n_kv) * sp_size + my_sp, 2**30)
        sm_ref[...] = jnp.zeros_like(sm_ref)
        sl_ref[...] = jnp.zeros_like(sl_ref)

    for b in range(2):
        ko_ref[0, b] = k_ref[0, b]
        vo_ref[0, b] = v_ref[0, b]
        length = meta[2 * pair + b]
        step = lax.rem(my_sp - lax.rem(length, sp_size) + sp_size, sp_size)
        slot = lax.div(length + step, sp_size)
        per = 16 // n_kv
        base = pl.multiple_of(lax.div(slot, per) * 16, 16)
        sub = lax.rem(slot, per)
        mine = lax.broadcasted_iota(jnp.int32, (16, hd), 0) // n_kv == sub
        ko_ref[0, b, pl.ds(base, 16), :] = jnp.where(mine, kn_ref[b], k_ref[0, b, pl.ds(base, 16), :])
        vo_ref[0, b, pl.ds(base, 16), :] = jnp.where(mine, vn_ref[b], v_ref[0, b, pl.ds(base, 16), :])

    q = q_ref[...].reshape(rows, hd)
    rcol = lax.broadcasted_iota(jnp.int32, (rows, 1), 0) % r8
    first = rcol < n_steps
    limit = jnp.where(first, meta[2 * pair], meta[2 * pair + 1]) + rcol % n_steps
    zero = jnp.zeros_like(q)
    q2 = jnp.concatenate([jnp.where(first, q, zero), jnp.where(first, zero, q)], axis=1).astype(BF16)
    k2 = jnp.concatenate([ko_ref[0, 0], ko_ref[0, 1]], axis=1)
    s = lax.dot_general(q2, k2, (((1,), (1,)), ((), ())), preferred_element_type=F32)
    s = jnp.where(code[...] <= limit, s * hd ** -0.5, -1e30)
    m = jnp.max(s, axis=-1, keepdims=True)
    p = jnp.exp(s - m)
    l = jnp.sum(p, axis=-1, keepdims=True)
    v2 = jnp.concatenate([vo_ref[0, 0], vo_ref[0, 1]], axis=1)
    o = jnp.dot(p.astype(BF16), v2, preferred_element_type=F32)
    o = jnp.where(first, o[:, :hd], o[:, hd:])
    o_ref[...] = o.reshape(heads, r8, hd)
    lane = lax.broadcasted_iota(jnp.int32, sm_ref.shape, 1)
    sm_ref[...] = jnp.where(lane == pair, m, sm_ref[...])
    sl_ref[...] = jnp.where(lane == pair, l, sl_ref[...])


def attn_call(layer, meta, q, kn, vn, kc, vc, prev, n_kv, n_steps, sp_size):
    n_layers, n_batch, n_cols, hd = kc.shape
    heads, rows, _ = q.shape
    r8 = 2 * n_steps
    srows = heads * r8
    cache = pl.BlockSpec((1, 2, n_cols, hd), lambda i, *_: (layer, i, 0, 0))
    in_specs = [
        pl.BlockSpec((heads, r8, hd), lambda i, *_: (0, i, 0)),
        pl.BlockSpec((2, 16, hd), lambda i, *_: (i, 0, 0)),
        pl.BlockSpec((2, 16, hd), lambda i, *_: (i, 0, 0)),
        cache, cache,
    ]
    args = [q, kn, vn, kc, vc]
    aliases = {}
    if prev is not None:
        in_specs += [pl.BlockSpec(memory_space=pl.ANY)] * 2
        args += list(prev)
        aliases = {6: 0, 7: 1}
    stat = pl.BlockSpec((srows, 128), lambda i, *_: (0, 0))
    return pl.pallas_call(
        functools.partial(attn_kernel, n_kv, n_steps, sp_size, prev is not None),
        grid_spec=pltpu.PrefetchScalarGridSpec(
            num_scalar_prefetch=1,
            grid=(n_batch // 2,),
            in_specs=in_specs,
            out_specs=[cache, cache, pl.BlockSpec((heads, r8, hd), lambda i, *_: (0, i, 0)), stat, stat],
            scratch_shapes=[pltpu.VMEM((srows, n_cols), jnp.int32)],
        ),
        out_shape=[
            jax.ShapeDtypeStruct(kc.shape, kc.dtype), jax.ShapeDtypeStruct(vc.shape, vc.dtype),
            jax.ShapeDtypeStruct((heads, rows, hd), F32),
            jax.ShapeDtypeStruct((srows, 128), F32), jax.ShapeDtypeStruct((srows, 128), F32),
        ],
        input_output_aliases=aliases,
        compiler_params=pltpu.CompilerParams(vmem_limit_bytes=40 * 2**20),
        name=f'attn{layer}',
    )(meta, *args)


def block_kernel(layer, o_ref, sm_ref, sl_ref, u_ref, gain_ref, wo_hbm, wg_hbm, wu_hbm, wd_hbm, out_ref,
                 wo_v, wg_v, wu_v, wd_v, part, g1, g2, h2, act, att,
                 r_d, r_x1, r_y1, r_x2, r_y2, r_o, r_st, mo_s, mo_k, mst, r_o2, r_st2,
                 wo_sem, wg_sem, wu_sem, wd_sem, m_send, m_recv, rs_send, rs_recv, ag_send, ag_recv):
    sp = lax.axis_index('sp')
    y = lax.axis_index('tp')
    c = lax.rem(sp, 2)
    x = lax.div(sp, 2)
    rows = u_ref.shape[0]
    d_model = u_ref.shape[1]
    hd = o_ref.shape[2]
    heads = o_ref.shape[0]
    n_pieces = d_model // PC
    f_loc = wd_v.shape[1]
    k_loc = wo_v.shape[1]
    n_f = wg_v.shape[0]
    core_dev = {'sp': 2 * x + 1 - c}
    x_dev = {'sp': 2 * (1 - x) + c}
    y_dev = {'tp': 1 - y}

    def piece(half, kind, far, sub):
        return half * 8 + kind * 4 + far * 2 + sub

    order = []
    for half in (1 - c, c):
        for kind, far in ((0, 1 - x), (1, 1 - y), (0, x), (1, y)):
            for sub in ((1 - y, y) if kind == 0 else (1 - x, x)):
                order.append(piece(half, kind, far, sub))

    copies = {}

    def start(key, src, dst, sem):
        cp = pltpu.make_async_copy(src, dst, sem)
        cp.start()
        copies[key] = cp

    rem_row = pl.multiple_of((8 * c + 4 * x) * hd, hd)
    for i in range(n_pieces):
        start(('o', i), wo_hbm.at[layer, pl.ds(rem_row, k_loc), pl.ds(pl.multiple_of(order[i] * PC, PC), PC)], wo_v.at[i], wo_sem.at[i])

    barrier = pltpu.get_barrier_semaphore()
    for dev in (core_dev, x_dev, y_dev):
        pl.semaphore_signal(barrier, inc=1, device_id=dev, device_id_type=MESH)
    pl.semaphore_wait(barrier, 3)

    def remote(src, dst, send, recv, dev):
        cp = pltpu.make_async_remote_copy(src_ref=src, dst_ref=dst, send_sem=send, recv_sem=recv, device_id=dev, device_id_type=MESH)
        cp.start()
        return cp

    hh = heads // 2
    hq = heads // 4
    sr = sm_ref.shape[0]
    away = 1 - c
    d_cp = [
        remote(sm_ref.at[pl.ds(pl.multiple_of(away * (sr // 2), 8), sr // 2)], r_st.at[0], m_send.at[0], m_recv.at[0], core_dev),
        remote(sl_ref.at[pl.ds(pl.multiple_of(away * (sr // 2), 8), sr // 2)], r_st.at[1], m_send.at[1], m_recv.at[1], core_dev),
        remote(o_ref.at[pl.ds(away * hh, hh)], r_o, m_send.at[2], m_recv.at[2], core_dev),
    ]

    f_off = pl.multiple_of(sp * f_loc, PC)
    for i in range(n_f):
        start(('g', i), wg_hbm.at[layer, :, pl.ds(pl.multiple_of(f_off + i * PC, PC), PC)], wg_v.at[i], wg_sem.at[i])
        start(('u', i), wu_hbm.at[layer, :, pl.ds(pl.multiple_of(f_off + i * PC, PC), PC)], wu_v.at[i], wu_sem.at[i])
    for i in range(n_pieces):
        start(('d', i), wd_hbm.at[layer, pl.ds(f_off, f_loc), pl.ds(pl.multiple_of(order[i] * PC, PC), PC)], wd_v.at[i], wd_sem.at[i])

    for cp in d_cp:
        cp.wait_recv()

    def merge_into(dst, st_dst, src_o, m1, l1, src_o2, m2, l2, n_heads):
        mx = jnp.maximum(m1, m2)
        f1 = jnp.exp(m1 - mx)
        f2 = jnp.exp(m2 - mx)
        ln = l1 * f1 + l2 * f2
        st_dst(mx, ln)
        for h in range(n_heads):
            for t in range(rows // 8):
                a = jnp.broadcast_to(f1[8 * h:8 * h + 8, t:t + 1], (8, hd))
                b = jnp.broadcast_to(f2[8 * h:8 * h + 8, t:t + 1], (8, hd))
                dst(h, t, src_o(h, t) * a + src_o2(h, t) * b, ln)

    def core_merge(q4, dst_o, slot):
        lo = pl.multiple_of(c * (sr // 2) + q4 * (sr // 4), 8)
        lr = pl.multiple_of(q4 * (sr // 4), 8)
        n = sr // 4

        def st_dst(mx, ln):
            mst[slot, 0] = mx
            mst[slot, 1] = ln

        def dst(h, t, val, ln):
            dst_o[h, 8 * t:8 * t + 8, :] = val

        merge_into(dst, st_dst,
                   lambda h, t: o_ref[c * hh + q4 * hq + h, 8 * t:8 * t + 8, :], sm_ref[pl.ds(lo, n)], sl_ref[pl.ds(lo, n)],
                   lambda h, t: r_o[q4 * hq + h, 8 * t:8 * t + 8, :], r_st[0, pl.ds(lr, n)], r_st[1, pl.ds(lr, n)], hq)

    core_merge(1 - x, mo_s, 0)
    x_cp = [
        remote(mst.at[0], r_st2, m_send.at[3], m_recv.at[3], x_dev),
        remote(mo_s, r_o2, m_send.at[4], m_recv.at[4], x_dev),
    ]
    core_merge(x, mo_k, 1)
    for cp in x_cp:
        cp.wait_recv()

    def fin(h, t, val, ln):
        den = jnp.broadcast_to(ln[8 * h:8 * h + 8, t:t + 1], (8, hd))
        mo_k[h, 8 * t:8 * t + 8, :] = val / den

    merge_into(fin, lambda mx, ln: None,
               lambda h, t: mo_k[h, 8 * t:8 * t + 8, :], mst[1, 0], mst[1, 1],
               lambda h, t: r_o2[h, 8 * t:8 * t + 8, :], r_st2[0], r_st2[1], hq)
    for h in range(hq):
        att[:, h * hd:(h + 1) * hd] = mo_k[h].astype(BF16)
    for cp in d_cp + x_cp:
        cp.wait_send()

    def all_reduce(product, resid, g):
        sends = []

        def rs(n, src, dst, dev):
            cp = remote(src, dst, rs_send.at[n], rs_recv.at[n], dev)
            sends.append(cp)
            return cp

        for k in range(4):
            for i in (2 * k, 2 * k + 1):
                part[i] = product(i)
            cp = rs(k, part.at[pl.ds(2 * k, 2)], r_d.at[pl.ds(2 * k, 2)], core_dev)
        waits = sends[:4]
        for k in range(4):
            for i in (2 * k, 2 * k + 1):
                part[8 + i] = product(8 + i)
            waits[k].wait_recv()
            for i in (2 * k, 2 * k + 1):
                part[8 + i] = part[8 + i] + r_d[i]
            if k == 0:
                a1 = rs(4, part.at[pl.ds(8, 2)], r_x1, x_dev)
            if k == 1:
                b1 = rs(5, part.at[pl.ds(10, 2)], r_y1, y_dev)
        a1.wait_recv()
        part[12] = part[12] + r_x1[0]
        a2 = rs(6, part.at[12], r_y2, y_dev)
        b1.wait_recv()
        part[14] = part[14] + r_y1[0]
        b2 = rs(7, part.at[14], r_x2, x_dev)
        part[13] = part[13] + r_x1[1]
        part[15] = part[15] + r_y1[1]

        gs = []

        def ag(n, p, dev):
            cp = remote(g.at[p], g.at[p], ag_send.at[n], ag_recv.at[n], dev)
            gs.append(cp)
            return cp

        pa = piece(c, 0, x, y)
        pb = piece(c, 1, y, x)
        a2.wait_recv()
        g[pa] = (resid(pa) + (part[13] + r_y2[...])).astype(BF16).astype(F32)
        ya = ag(0, pa, y_dev)
        xa = ag(1, pa, x_dev)
        d0 = ag(2, pa, core_dev)
        b2.wait_recv()
        g[pb] = (resid(pb) + (part[15] + r_x2[...])).astype(BF16).astype(F32)
        xb = ag(3, pb, x_dev)
        yb = ag(4, pb, y_dev)
        d1 = ag(5, pb, core_dev)
        ya.wait_recv()
        p = piece(c, 0, x, 1 - y)
        xf = ag(6, p, x_dev)
        d2 = ag(7, p, core_dev)
        xb.wait_recv()
        p = piece(c, 1, y, 1 - x)
        yf = ag(8, p, y_dev)
        d3 = ag(9, p, core_dev)
        xa.wait_recv()
        d4 = ag(10, piece(c, 0, 1 - x, y), core_dev)
        yb.wait_recv()
        d5 = ag(11, piece(c, 1, 1 - y, x), core_dev)
        xf.wait_recv()
        d6 = ag(12, piece(c, 0, 1 - x, 1 - y), core_dev)
        yf.wait_recv()
        d7 = ag(13, piece(c, 1, 1 - y, 1 - x), core_dev)
        for cp in (d0, d1, d2, d3, d4, d5, d6, d7):
            cp.wait_recv()
        for cp in sends + gs:
            cp.wait_send()

    def out_product(i):
        copies[('o', i)].wait()
        return jnp.dot(att[...], wo_v[i], preferred_element_type=F32)

    def u_resid(p):
        return u_ref[:, pl.ds(pl.multiple_of(p * PC, PC), PC)].astype(F32)

    all_reduce(out_product, u_resid, g1)

    sq = jnp.zeros((rows, PC), F32)
    for i in range(n_pieces):
        sq = sq + g1[i] * g1[i]
    inv = lax.rsqrt(jnp.sum(sq, axis=-1, keepdims=True) * (1.0 / d_model) + EPS)
    for i in range(n_pieces):
        h2[:, i * PC:(i + 1) * PC] = (g1[i] * inv * gain_ref[:, i * PC:(i + 1) * PC].astype(F32)).astype(BF16)

    for i in range(n_f):
        copies[('g', i)].wait()
        ga = jnp.dot(h2[...], wg_v[i], preferred_element_type=F32)
        copies[('u', i)].wait()
        up = jnp.dot(h2[...], wu_v[i], preferred_element_type=F32)
        act[:, i * PC:(i + 1) * PC] = (ga * jax.nn.sigmoid(ga) * up).astype(BF16)

    def down_product(i):
        copies[('d', i)].wait()
        return jnp.dot(act[...], wd_v[i], preferred_element_type=F32)

    all_reduce(down_product, lambda p: g1[p], g2)
    for i in range(n_pieces):
        out_ref[:, i * PC:(i + 1) * PC] = g2[i].astype(BF16)


def block_call(layer, o, sm, sl, u, gain, wo, wg, wu, wd, sp_size):
    rows, d_model = u.shape
    heads, _, hd = o.shape
    n_p = d_model // PC
    k_loc = wo.shape[1] // sp_size
    f_loc = wd.shape[1] // sp_size
    n_f = f_loc // PC
    sr = sm.shape[0]
    V = pltpu.VMEM
    dma = pltpu.SemaphoreType.DMA
    vm = pl.BlockSpec(memory_space=pltpu.VMEM)
    hbm = pl.BlockSpec(memory_space=pl.ANY)
    return pl.pallas_call(
        functools.partial(block_kernel, layer),
        out_shape=jax.ShapeDtypeStruct((rows, d_model), BF16),
        in_specs=[vm] * 5 + [hbm] * 4,
        out_specs=vm,
        scratch_shapes=[
            V((n_p, k_loc, PC), BF16), V((n_f, d_model, PC), BF16), V((n_f, d_model, PC), BF16), V((n_p, f_loc, PC), BF16),
            V((n_p, rows, PC), F32), V((n_p, rows, PC), F32), V((n_p, rows, PC), F32),
            V((rows, d_model), BF16), V((rows, f_loc), BF16), V((rows, k_loc), BF16),
            V((n_p // 2, rows, PC), F32), V((2, rows, PC), F32), V((2, rows, PC), F32), V((rows, PC), F32), V((rows, PC), F32),
            V((heads // 2, rows, hd), F32), V((2, sr // 2, 128), F32),
            V((heads // 4, rows, hd), F32), V((heads // 4, rows, hd), F32), V((2, 2, sr // 4, 128), F32),
            V((heads // 4, rows, hd), F32), V((2, sr // 4, 128), F32),
            dma((n_p,)), dma((n_f,)), dma((n_f,)), dma((n_p,)),
            dma((5,)), dma((5,)), dma((8,)), dma((8,)), dma((14,)), dma((14,)),
        ],
        compiler_params=pltpu.CompilerParams(collective_id=layer, has_side_effects=True, vmem_limit_bytes=67043328),
        name=f'block{layer}',
    )(o, sm, sl, u, gain, wo, wg, wu, wd)


def solution(mesh):
    sp_size = mesh.shape['sp']

    def local_fn(tok_emb, lengths, key_cache, val_cache, gain_attn, gain_mlp, w_query, w_key, w_value, w_out, w_gate, w_up, w_down):
        n_steps, n_batch, d_model = tok_emb.shape
        n_layers, _, loc_len, kv_loc, hd = key_cache.shape
        rows = n_steps * n_batch
        my_sp = lax.axis_index('sp').astype(jnp.int32)
        cur_pos = (lengths[:, None] + jnp.arange(n_steps)[None, :]).reshape(rows)
        cos_a, sin_a = rope_tables(cur_pos, hd)
        mine = (cur_pos % sp_size == my_sp).reshape(n_batch, n_steps)
        meta = jnp.concatenate([lengths, my_sp[None]])
        u = tok_emb.transpose(1, 0, 2).reshape(rows, d_model)
        kc = key_cache.reshape(n_layers, n_batch, loc_len * kv_loc, hd)
        vc = val_cache.reshape(n_layers, n_batch, loc_len * kv_loc, hd)

        def own_row(t):
            t = t.reshape(kv_loc, n_batch, n_steps, hd)
            t = jnp.sum(jnp.where(mine[None, :, :, None], t, jnp.zeros_like(t)), axis=2)
            return jnp.tile(t.transpose(1, 0, 2), (1, 16 // kv_loc, 1))

        prev = None
        for layer in range(n_layers):
            q, k, v = qkv_call(layer, u, gain_attn[layer][None], cos_a, sin_a, w_query, w_key, w_value, hd)
            nk, nv, o, sm, sl = attn_call(layer, meta, q, own_row(k), own_row(v), kc, vc, prev, kv_loc, n_steps, sp_size)
            prev = (nk, nv)
            u = block_call(layer, o, sm, sl, u, gain_mlp[layer][None], w_out, w_gate, w_up, w_down, sp_size)
        hidden = u.reshape(n_batch, n_steps, d_model).transpose(1, 0, 2)
        return hidden, prev[0].reshape(key_cache.shape), prev[1].reshape(val_cache.shape)

    cache_spec = P(None, 'dp', 'sp', 'tp', None)
    col_spec = P(None, None, 'tp')
    row_spec = P(None, 'tp', None)
    emb_spec = P(None, 'dp', None)
    return jax.shard_map(local_fn, mesh=mesh, in_specs=(emb_spec, P('dp'), cache_spec, cache_spec, P(), P(), col_spec, col_spec, col_spec, row_spec, col_spec, col_spec, row_spec), out_specs=(emb_spec, cache_spec, cache_spec), check_vma=False)
```

```python
import functools

import jax
import jax.numpy as jnp
import numpy as np
from jax import lax
from jax.experimental import pallas as pl
from jax.experimental.pallas import tpu as pltpu
from jax.sharding import PartitionSpec as P

EPS = 1e-5
ROPE_BASE = 500000.0
F32 = jnp.float32
BF16 = jnp.bfloat16
MESH = pl.DeviceIdType.MESH
PC = 256
VMEM_ALL = 67043328


def rope_table(first_pos, n_pos, head_dim):
    half = head_dim // 2
    inv_freq = (1.0 / (np.float32(ROPE_BASE) ** (np.arange(half).astype(np.float32) * np.float32(2.0 / head_dim)))).astype(np.float32)
    pos = np.arange(first_pos, first_pos + n_pos).astype(np.float32)
    angles = (pos[:, None] * inv_freq[None, :]).astype(np.float32)
    return np.concatenate([np.cos(angles), np.sin(angles)], axis=1).astype(np.float32)


def permutation(rows, n_steps, to_batch_major):
    ri = lax.broadcasted_iota(jnp.int32, (rows, rows), 0)
    ci = lax.broadcasted_iota(jnp.int32, (rows, rows), 1)
    n_batch = rows // n_steps
    if to_batch_major:
        src = (ri % n_steps) * n_batch + ri // n_steps
    else:
        src = (ri % n_batch) * n_steps + ri // n_batch
    return jnp.where(ci == src, 1.0, 0.0).astype(BF16)


def qkv_kernel(layer, n_steps, first_pos, first, *refs):
    if first:
        len_ref, tab_ref, u_ref, gain_ref, wq_ref, wk_ref, wv_ref, q_ref, k_ref, v_ref, cos_ref, sin_ref, up_ref, h_scr = refs
    else:
        u_ref, gain_ref, cos_ref, sin_ref, wq_ref, wk_ref, wv_ref, q_ref, k_ref, v_ref, h_scr = refs
    rows, d_model = u_ref.shape
    hd = cos_ref.shape[1]

    @pl.when(pl.program_id(0) == 0)
    def _():
        x = u_ref[...].astype(F32)
        inv = lax.rsqrt(jnp.sum(x * x, axis=-1, keepdims=True) * (1.0 / d_model) + EPS)
        h = (x * inv * gain_ref[layer:layer + 1, :].astype(F32)).astype(BF16)
        if first:
            perm = permutation(rows, n_steps, True)
            h_scr[...] = jnp.dot(perm, h, preferred_element_type=F32).astype(BF16)
            up_ref[...] = jnp.dot(perm, u_ref[...], preferred_element_type=F32).astype(BF16)
            for b in range(rows // n_steps):
                cos_ref[b * n_steps:(b + 1) * n_steps, :] = tab_ref[pl.ds(len_ref[b] - first_pos, n_steps), :]
            both = cos_ref[...]
            swap = pltpu.roll(both, hd // 2, 1)
            low = lax.broadcasted_iota(jnp.int32, both.shape, 1) < hd // 2
            cos_ref[...] = jnp.where(low, both, swap)
            sin_ref[...] = jnp.where(low, -swap, both)
        else:
            h_scr[...] = h

    h = h_scr[...]
    cos_a, sin_a = cos_ref[...], sin_ref[...]

    def rot(x):
        return (x * cos_a + pltpu.roll(x, hd // 2, 1) * sin_a).astype(BF16).astype(F32)

    q = jnp.dot(h, wq_ref[0], preferred_element_type=F32)
    for j in range(q_ref.shape[0]):
        q_ref[j] = rot(q[:, j * hd:(j + 1) * hd])
    k = jnp.dot(h, wk_ref[0], preferred_element_type=F32)
    k_ref[0] = rot(k)
    v = jnp.dot(h, wv_ref[0], preferred_element_type=F32)
    v_ref[0] = v.astype(BF16).astype(F32)


def qkv_call(layer, u, gain, rope, lengths, wq, wk, wv, n_steps, hd, first_pos):
    rows, d_model = u.shape
    kv_loc = wk.shape[2] // hd
    heads = wq.shape[2] // hd
    grp = heads // kv_loc
    first = layer == 0
    full = lambda shape: pl.BlockSpec(shape, lambda j: (0,) * len(shape))
    weights = [
        pl.BlockSpec((1, d_model, grp * hd), lambda j: (layer, 0, j)),
        pl.BlockSpec((1, d_model, hd), lambda j: (layer, 0, j)),
        pl.BlockSpec((1, d_model, hd), lambda j: (layer, 0, j)),
    ]
    out_specs = [
        pl.BlockSpec((grp, rows, hd), lambda j: (j, 0, 0)),
        pl.BlockSpec((1, rows, hd), lambda j: (j, 0, 0)),
        pl.BlockSpec((1, rows, hd), lambda j: (j, 0, 0)),
    ]
    out_shape = [
        jax.ShapeDtypeStruct((heads, rows, hd), F32),
        jax.ShapeDtypeStruct((kv_loc, rows, hd), F32),
        jax.ShapeDtypeStruct((kv_loc, rows, hd), F32),
    ]
    if first:
        args = [lengths, rope, u, gain, wq, wk, wv]
        in_specs = [pl.BlockSpec(memory_space=pltpu.SMEM), full(rope.shape), full(u.shape), full(gain.shape)] + weights
        out_specs += [full((rows, hd)), full((rows, hd)), full((rows, d_model))]
        out_shape += [jax.ShapeDtypeStruct((rows, hd), F32)] * 2 + [jax.ShapeDtypeStruct((rows, d_model), BF16)]
    else:
        args = [u, gain, *rope, wq, wk, wv]
        in_specs = [full(u.shape), full(gain.shape), full((rows, hd)), full((rows, hd))] + weights
    return pl.pallas_call(
        functools.partial(qkv_kernel, layer, n_steps, first_pos, first),
        grid=(kv_loc,),
        in_specs=in_specs,
        out_specs=out_specs,
        out_shape=out_shape,
        scratch_shapes=[pltpu.VMEM((rows, d_model), BF16)],
        compiler_params=pltpu.CompilerParams(vmem_limit_bytes=VMEM_ALL),
        name=f'qkv{layer}',
    )(*args)


SEQS = 4
SLOTS = 6
AHEAD = 4


def attn_kernel(layer, n_kv, n_steps, sp_size, has_prev, len_ref, q_ref, kn_ref, vn_ref, k_hbm, v_hbm, *rest):
    if has_prev:
        rest = rest[2:]
    ko_hbm, vo_hbm, o_ref, sm_ref, sl_ref, code, kb, vb, in_sem, out_sem = rest
    my_sp = lax.axis_index('sp').astype(jnp.int32)
    heads, all_rows, hd = q_ref.shape
    n_batch = all_rows // n_steps
    n_iter = n_batch // SEQS
    r8 = 2 * n_steps
    rows = heads * r8
    n_cols = kb.shape[2]
    row_kv = rows // n_kv

    def reads(i):
        slot = lax.rem(i, SLOTS)
        src = pl.ds(i * SEQS, SEQS)
        return (pltpu.make_async_copy(k_hbm.at[layer, src], kb.at[slot], in_sem.at[slot, 0]),
                pltpu.make_async_copy(v_hbm.at[layer, src], vb.at[slot], in_sem.at[slot, 1]))

    def writes(i):
        slot = lax.rem(i, SLOTS)
        dst = pl.ds(i * SEQS, SEQS)
        return (pltpu.make_async_copy(kb.at[slot], ko_hbm.at[layer, dst], out_sem.at[slot, 0]),
                pltpu.make_async_copy(vb.at[slot], vo_hbm.at[layer, dst], out_sem.at[slot, 1]))

    for i in range(AHEAD):
        for cp in reads(i):
            cp.start()

    ri = lax.broadcasted_iota(jnp.int32, (rows, n_cols), 0)
    ci = lax.broadcasted_iota(jnp.int32, (rows, n_cols), 1)
    same = (ci % n_kv) == (ri // row_kv)
    code[...] = jnp.where(same, (ci // n_kv) * sp_size + my_sp, 2**30)
    sm_ref[...] = jnp.zeros_like(sm_ref)
    sl_ref[...] = jnp.zeros_like(sl_ref)
    rcol = lax.broadcasted_iota(jnp.int32, (rows, 1), 0) % r8
    first = rcol < n_steps
    row16 = lax.broadcasted_iota(jnp.int32, (16, hd), 0)
    lane = lax.broadcasted_iota(jnp.int32, sm_ref.shape, 1)
    per = 16 // n_kv

    def body(i, _):
        slot_b = lax.rem(i, SLOTS)
        for cp in reads(i):
            cp.wait()
        for b in range(SEQS):
            seq = i * SEQS + b
            length = len_ref[seq]
            step = lax.rem(my_sp - lax.rem(length, sp_size) + sp_size, sp_size)
            slot = lax.div(length + step, sp_size)
            base = pl.multiple_of(lax.div(slot, per) * 16, 16)
            mine = row16 // n_kv == lax.rem(slot, per)
            new_row = seq * n_steps + step
            for buf, src in ((kb, kn_ref), (vb, vn_ref)):
                fresh = jnp.broadcast_to(src[0, pl.ds(new_row, 1), :], (16, hd))
                for j in range(1, n_kv):
                    fresh = jnp.where(row16 % n_kv == j, jnp.broadcast_to(src[j, pl.ds(new_row, 1), :], (16, hd)), fresh)
                old = buf[slot_b, b, pl.ds(base, 16), :]
                buf[slot_b, b, pl.ds(base, 16), :] = jnp.where(mine, fresh, old.astype(F32)).astype(BF16)
        for cp in writes(i):
            cp.start()
        sm, sl = sm_ref[...], sl_ref[...]
        for t in range(SEQS // 2):
            pair = i * (SEQS // 2) + t
            r0 = pl.multiple_of(pair * r8, r8)
            q = q_ref[:, pl.ds(r0, r8), :].reshape(rows, hd)
            limit = jnp.where(first, len_ref[2 * pair], len_ref[2 * pair + 1]) + rcol % n_steps
            zero = jnp.zeros_like(q)
            q2 = jnp.concatenate([jnp.where(first, q, zero), jnp.where(first, zero, q)], axis=1).astype(BF16)
            k2 = jnp.concatenate([kb[slot_b, 2 * t], kb[slot_b, 2 * t + 1]], axis=1)
            s = lax.dot_general(q2, k2, (((1,), (1,)), ((), ())), preferred_element_type=F32)
            s = jnp.where(code[...] <= limit, s * hd ** -0.5, -1e30)
            m = jnp.max(s, axis=-1, keepdims=True)
            p = jnp.exp(s - m)
            l = jnp.sum(p, axis=-1, keepdims=True)
            v2 = jnp.concatenate([vb[slot_b, 2 * t], vb[slot_b, 2 * t + 1]], axis=1)
            o = jnp.dot(p.astype(BF16), v2, preferred_element_type=F32)
            o = jnp.where(first, o[:, :hd], o[:, hd:])
            o_ref[:, pl.ds(r0, r8), :] = o.reshape(heads, r8, hd)
            sm = jnp.where(lane == pair, m, sm)
            sl = jnp.where(lane == pair, l, sl)
        sm_ref[...] = sm
        sl_ref[...] = sl

        @pl.when(i + AHEAD >= SLOTS)
        def _():
            for cp in writes(i + AHEAD - SLOTS):
                cp.wait()

        @pl.when(i + AHEAD < n_iter)
        def _():
            for cp in reads(i + AHEAD):
                cp.start()
        return 0

    lax.fori_loop(0, n_iter, body, 0)
    for i in range(n_iter + AHEAD - SLOTS, n_iter):
        for cp in writes(i):
            cp.wait()


def attn_call(layer, lengths, q, kn, vn, kc, vc, prev, n_kv, n_steps, sp_size):
    n_layers, n_batch, n_cols, hd = kc.shape
    heads, rows, _ = q.shape
    srows = heads * 2 * n_steps
    vm = pl.BlockSpec(memory_space=pltpu.VMEM)
    hbm = pl.BlockSpec(memory_space=pl.ANY)
    in_specs = [pl.BlockSpec(memory_space=pltpu.SMEM), vm, vm, vm, hbm, hbm]
    args = [lengths, q, kn, vn, kc, vc]
    aliases = {}
    if prev is not None:
        in_specs += [hbm, hbm]
        args += list(prev)
        aliases = {6: 0, 7: 1}
    return pl.pallas_call(
        functools.partial(attn_kernel, layer, n_kv, n_steps, sp_size, prev is not None),
        in_specs=in_specs,
        out_specs=[hbm, hbm, vm, vm, vm],
        out_shape=[
            jax.ShapeDtypeStruct(kc.shape, kc.dtype), jax.ShapeDtypeStruct(vc.shape, vc.dtype),
            jax.ShapeDtypeStruct((heads, rows, hd), F32),
            jax.ShapeDtypeStruct((srows, 128), F32), jax.ShapeDtypeStruct((srows, 128), F32),
        ],
        scratch_shapes=[
            pltpu.VMEM((srows, n_cols), jnp.int32),
            pltpu.VMEM((SLOTS, SEQS, n_cols, hd), BF16), pltpu.VMEM((SLOTS, SEQS, n_cols, hd), BF16),
            pltpu.SemaphoreType.DMA((SLOTS, 2)), pltpu.SemaphoreType.DMA((SLOTS, 2)),
        ],
        input_output_aliases=aliases,
        compiler_params=pltpu.CompilerParams(vmem_limit_bytes=VMEM_ALL),
        name=f'attn{layer}',
    )(*args)


def block_kernel(layer, last, n_steps, o_ref, sm_ref, sl_ref, u_ref, gain_ref, wo_hbm, wg_hbm, wu_hbm, wd_hbm, *refs):
    has_next = not last
    if has_next:
        gain_a_ref, cos_ref, sin_ref, wq_hbm, wk_hbm, wv_hbm, out_ref, q_ref, k_ref, v_ref, *refs = refs
    else:
        out_ref, *refs = refs
    block_body(layer, last, n_steps, has_next, o_ref, sm_ref, sl_ref, u_ref, gain_ref, wo_hbm, wg_hbm, wu_hbm, wd_hbm,
               (gain_a_ref, cos_ref, sin_ref, wq_hbm, wk_hbm, wv_hbm) if has_next else None, out_ref,
               (q_ref, k_ref, v_ref) if has_next else None, *refs)


def block_body(layer, last, n_steps, has_next, o_ref, sm_ref, sl_ref, u_ref, gain_ref, wo_hbm, wg_hbm, wu_hbm, wd_hbm, nxt, out_ref, qkv,
                 wo_v, wg_v, wu_v, wd_v, part, g1, g2, h2, act, att,
                 r_d, r_x1, r_y1, r_x2, r_y2, r_o, r_st, mo_s, mo_k, mst, r_o2, r_st2,
                 wo_sem, wg_sem, wu_sem, wd_sem, m_send, m_recv, rs_send, rs_recv, ag_send, ag_recv):
    if has_next:
        gain_a_ref, cos_ref, sin_ref, wq_hbm, wk_hbm, wv_hbm = nxt
        q_ref, k_ref, v_ref = qkv
    sp = lax.axis_index('sp')
    y = lax.axis_index('tp')
    c = lax.rem(sp, 2)
    x = lax.div(sp, 2)
    rows = u_ref.shape[0]
    d_model = u_ref.shape[1]
    hd = o_ref.shape[2]
    heads = o_ref.shape[0]
    n_pieces = d_model // PC
    f_loc = wd_v.shape[1]
    k_loc = wo_v.shape[1]
    n_f = wg_v.shape[0]
    core_dev = {'sp': 2 * x + 1 - c}
    x_dev = {'sp': 2 * (1 - x) + c}
    y_dev = {'tp': 1 - y}

    def piece(half, kind, far, sub):
        return half * 8 + kind * 4 + far * 2 + sub

    order = []
    for far_x, far_y in ((1 - x, 1 - y), (x, y)):
        for half in (1 - c, c):
            for kind, far in ((0, far_x), (1, far_y)):
                for sub in ((1 - y, y) if kind == 0 else (1 - x, x)):
                    order.append(piece(half, kind, far, sub))

    copies = {}

    def start(key, src, dst, sem):
        cp = pltpu.make_async_copy(src, dst, sem)
        cp.start()
        copies[key] = cp

    rem_row = pl.multiple_of((8 * c + 4 * x) * hd, hd)
    for i in range(n_pieces):
        start(('o', i), wo_hbm.at[layer, pl.ds(rem_row, k_loc), pl.ds(pl.multiple_of(order[i] * PC, PC), PC)], wo_v.at[i], wo_sem.at[i])

    barrier = pltpu.get_barrier_semaphore()
    for dev in (core_dev, x_dev, y_dev):
        pl.semaphore_signal(barrier, inc=1, device_id=dev, device_id_type=MESH)
    pl.semaphore_wait(barrier, 3)

    def remote(src, dst, send, recv, dev):
        cp = pltpu.make_async_remote_copy(src_ref=src, dst_ref=dst, send_sem=send, recv_sem=recv, device_id=dev, device_id_type=MESH)
        cp.start()
        return cp

    hh = heads // 2
    hq = heads // 4
    sr = sm_ref.shape[0]
    away = 1 - c
    d_cp = [
        remote(sm_ref.at[pl.ds(pl.multiple_of(away * (sr // 2), 8), sr // 2)], r_st.at[0], m_send.at[0], m_recv.at[0], core_dev),
        remote(sl_ref.at[pl.ds(pl.multiple_of(away * (sr // 2), 8), sr // 2)], r_st.at[1], m_send.at[1], m_recv.at[1], core_dev),
        remote(o_ref.at[pl.ds(away * hh, hh)], r_o, m_send.at[2], m_recv.at[2], core_dev),
    ]

    f_off = pl.multiple_of(sp * f_loc, PC)
    def gate_copy(i):
        col = pl.ds(pl.multiple_of(f_off + i * PC, PC), PC)
        return (pltpu.make_async_copy(wg_hbm.at[layer, :, col], wg_v.at[i], wg_sem.at[i]),
                pltpu.make_async_copy(wu_hbm.at[layer, :, col], wu_v.at[i], wu_sem.at[i]))

    for i in range(n_f):
        for cp in gate_copy(i):
            cp.start()
    for i in range(n_pieces):
        start(('d', i), wd_hbm.at[layer, pl.ds(f_off, f_loc), pl.ds(pl.multiple_of(order[i] * PC, PC), PC)], wd_v.at[i], wd_sem.at[i])

    for cp in d_cp:
        cp.wait_recv()

    def merge_into(dst, st_dst, src_o, m1, l1, src_o2, m2, l2, n_heads):
        mx = jnp.maximum(m1, m2)
        f1 = jnp.exp(m1 - mx)
        f2 = jnp.exp(m2 - mx)
        ln = l1 * f1 + l2 * f2
        st_dst(mx, ln)
        for h in range(n_heads):
            for t in range(rows // 8):
                a = jnp.broadcast_to(f1[8 * h:8 * h + 8, t:t + 1], (8, hd))
                b = jnp.broadcast_to(f2[8 * h:8 * h + 8, t:t + 1], (8, hd))
                dst(h, t, src_o(h, t) * a + src_o2(h, t) * b, ln)

    def core_merge(q4, dst_o, slot):
        lo = pl.multiple_of(c * (sr // 2) + q4 * (sr // 4), 8)
        lr = pl.multiple_of(q4 * (sr // 4), 8)
        n = sr // 4

        def st_dst(mx, ln):
            mst[slot, 0] = mx
            mst[slot, 1] = ln

        def dst(h, t, val, ln):
            dst_o[h, 8 * t:8 * t + 8, :] = val

        merge_into(dst, st_dst,
                   lambda h, t: o_ref[c * hh + q4 * hq + h, 8 * t:8 * t + 8, :], sm_ref[pl.ds(lo, n)], sl_ref[pl.ds(lo, n)],
                   lambda h, t: r_o[q4 * hq + h, 8 * t:8 * t + 8, :], r_st[0, pl.ds(lr, n)], r_st[1, pl.ds(lr, n)], hq)

    core_merge(1 - x, mo_s, 0)
    x_cp = [
        remote(mst.at[0], r_st2, m_send.at[3], m_recv.at[3], x_dev),
        remote(mo_s, r_o2, m_send.at[4], m_recv.at[4], x_dev),
    ]
    core_merge(x, mo_k, 1)
    for cp in x_cp:
        cp.wait_recv()

    def fin(h, t, val, ln):
        den = jnp.broadcast_to(ln[8 * h:8 * h + 8, t:t + 1], (8, hd))
        mo_k[h, 8 * t:8 * t + 8, :] = val / den

    merge_into(fin, lambda mx, ln: None,
               lambda h, t: mo_k[h, 8 * t:8 * t + 8, :], mst[1, 0], mst[1, 1],
               lambda h, t: r_o2[h, 8 * t:8 * t + 8, :], r_st2[0], r_st2[1], hq)
    for h in range(hq):
        att[:, h * hd:(h + 1) * hd] = mo_k[h].astype(BF16)
    for cp in d_cp + x_cp:
        cp.wait_send()

    def all_reduce(product, resid, g):
        sends = []

        def rs(n, src, dst, dev):
            cp = remote(src, dst, rs_send.at[n], rs_recv.at[n], dev)
            sends.append(cp)
            return cp

        def core_part(first, at):
            out = []
            for k in range(2):
                for i in (first + 2 * k, first + 2 * k + 1):
                    part[i] = product(i)
                out.append(rs(at // 2 + k, part.at[pl.ds(first + 2 * k, 2)], r_d.at[pl.ds(at + 2 * k, 2)], core_dev))
            return out

        d_in = core_part(0, 0)
        link = []
        for k, (buf, dev) in enumerate(((r_x1, x_dev), (r_y1, y_dev))):
            for j in range(2):
                i = 4 + 2 * k + j
                part[i] = product(i)
                if j == 0:
                    d_in[k].wait_recv()
                part[i] = part[i] + r_d[2 * k + j]
                link.append(rs(4 + 2 * k + j, part.at[i], buf.at[j], dev))
        d_in = core_part(8, 4)
        for k in range(2):
            for j in range(2):
                i = 12 + 2 * k + j
                part[i] = product(i)
                if j == 0:
                    d_in[k].wait_recv()
                part[i] = part[i] + r_d[4 + 2 * k + j]
        link[0].wait_recv()
        part[12] = part[12] + r_x1[0]
        a2 = rs(8, part.at[12], r_y2, y_dev)
        link[2].wait_recv()
        part[14] = part[14] + r_y1[0]
        b2 = rs(9, part.at[14], r_x2, x_dev)
        link[1].wait_recv()
        part[13] = part[13] + r_x1[1]
        link[3].wait_recv()
        part[15] = part[15] + r_y1[1]

        gs = []

        def ag(n, p, dev):
            cp = remote(g.at[p], g.at[p], ag_send.at[n], ag_recv.at[n], dev)
            gs.append(cp)
            return cp

        pa = piece(c, 0, x, y)
        pb = piece(c, 1, y, x)
        a2.wait_recv()
        g[pa] = (resid(pa) + (part[13] + r_y2[...])).astype(BF16).astype(F32)
        ya = ag(0, pa, y_dev)
        b2.wait_recv()
        g[pb] = (resid(pb) + (part[15] + r_x2[...])).astype(BF16).astype(F32)
        xb = ag(3, pb, x_dev)
        xa = ag(1, pa, x_dev)
        yb = ag(4, pb, y_dev)
        d0 = ag(2, pa, core_dev)
        d1 = ag(5, pb, core_dev)
        ya.wait_recv()
        p = piece(c, 0, x, 1 - y)
        xf = ag(6, p, x_dev)
        d2 = ag(7, p, core_dev)
        xb.wait_recv()
        p = piece(c, 1, y, 1 - x)
        yf = ag(8, p, y_dev)
        d3 = ag(9, p, core_dev)
        xa.wait_recv()
        d4 = ag(10, piece(c, 0, 1 - x, y), core_dev)
        yb.wait_recv()
        d5 = ag(11, piece(c, 1, 1 - y, x), core_dev)
        xf.wait_recv()
        d6 = ag(12, piece(c, 0, 1 - x, 1 - y), core_dev)
        yf.wait_recv()
        d7 = ag(13, piece(c, 1, 1 - y, 1 - x), core_dev)
        for cp in (d0, d1, d2, d3, d4, d5, d6, d7):
            cp.wait_recv()
        for cp in sends + gs:
            cp.wait_send()

    def out_product(i):
        copies[('o', i)].wait()
        return jnp.dot(att[...], wo_v[i], preferred_element_type=F32)

    def u_resid(p):
        return u_ref[:, pl.ds(pl.multiple_of(p * PC, PC), PC)].astype(F32)

    all_reduce(out_product, u_resid, g1)

    def norm(g, gains, row):
        sq = jnp.zeros((rows, PC), F32)
        for i in range(n_pieces):
            sq = sq + g[i] * g[i]
        inv = lax.rsqrt(jnp.sum(sq, axis=-1, keepdims=True) * (1.0 / d_model) + EPS)
        for i in range(n_pieces):
            cols = slice(i * PC, (i + 1) * PC)
            h2[:, cols] = (g[i] * inv * gains[row:row + 1, cols].astype(F32)).astype(BF16)

    norm(g1, gain_ref, layer)

    def gate_up(i, _):
        cg, cu = gate_copy(i)
        cg.wait()
        ga = jnp.dot(h2[...], wg_v[i], preferred_element_type=F32)
        cu.wait()
        up = jnp.dot(h2[...], wu_v[i], preferred_element_type=F32)
        act[:, pl.ds(pl.multiple_of(i * PC, PC), PC)] = (ga * jax.nn.sigmoid(ga) * up).astype(BF16)
        return 0

    lax.fori_loop(0, n_f, gate_up, 0)

    n_q = q_ref.shape[0] * hd // (2 * PC) if has_next else 0

    def next_copy(j):
        out = []
        for t, (buf, sem) in enumerate(((wg_v, wg_sem), (wu_v, wu_sem))):
            if isinstance(j, int) and j >= n_q:
                src = (wk_hbm, wv_hbm)[j - n_q].at[layer + 1, :, t * PC:(t + 1) * PC]
            else:
                src = wq_hbm.at[layer + 1, :, pl.ds(pl.multiple_of((2 * j + t) * PC, PC), PC)]
            out.append(pltpu.make_async_copy(src, buf.at[j], sem.at[j]))
        return out

    if has_next:
        for j in range(n_q + 2):
            for cp in next_copy(j):
                cp.start()

    def down_product(i):
        copies[('d', i)].wait()
        return jnp.dot(act[...], wd_v[i], preferred_element_type=F32)

    all_reduce(down_product, lambda p: g1[p], g2)
    back = permutation(rows, n_steps, False) if last else None
    for i in range(n_pieces):
        val = g2[i].astype(BF16)
        if last:
            val = jnp.dot(back, val, preferred_element_type=F32).astype(BF16)
        out_ref[:, i * PC:(i + 1) * PC] = val

    if has_next:
        norm(g2, gain_a_ref, layer + 1)
        cos_a, sin_a = cos_ref[...], sin_ref[...]

        def rot(z):
            return (z * cos_a + pltpu.roll(z, hd // 2, 1) * sin_a).astype(BF16).astype(F32)

        def heads_of(j, store):
            for t, (buf, cp) in enumerate(zip((wg_v, wu_v), next_copy(j))):
                cp.wait()
                val = jnp.dot(h2[...], buf[j], preferred_element_type=F32)
                for e in range(PC // hd):
                    store(t * (PC // hd) + e, val[:, e * hd:(e + 1) * hd])

        def q_pair(j, _):
            def store(e, val):
                q_ref[2 * (PC // hd) * j + e] = rot(val)
            heads_of(j, store)
            return 0

        def store_k(e, val):
            k_ref[e] = rot(val)

        def store_v(e, val):
            v_ref[e] = val.astype(BF16).astype(F32)

        lax.fori_loop(0, n_q, q_pair, 0)
        heads_of(n_q, store_k)
        heads_of(n_q + 1, store_v)


def block_call(layer, last, n_steps, o, sm, sl, u, gain, wo, wg, wu, wd, sp_size, nxt):
    rows, d_model = u.shape
    heads, _, hd = o.shape
    n_p = d_model // PC
    k_loc = wo.shape[1] // sp_size
    f_loc = wd.shape[1] // sp_size
    n_f = f_loc // PC
    sr = sm.shape[0]
    V = pltpu.VMEM
    dma = pltpu.SemaphoreType.DMA
    vm = pl.BlockSpec(memory_space=pltpu.VMEM)
    hbm = pl.BlockSpec(memory_space=pl.ANY)
    return pl.pallas_call(
        functools.partial(block_kernel, layer, last, n_steps),
        out_shape=[jax.ShapeDtypeStruct((rows, d_model), BF16)] + ([] if last else [
            jax.ShapeDtypeStruct((heads, rows, hd), F32),
            jax.ShapeDtypeStruct((nxt[4].shape[2] // hd, rows, hd), F32),
            jax.ShapeDtypeStruct((nxt[4].shape[2] // hd, rows, hd), F32)]),
        in_specs=[vm] * 5 + [hbm] * 4 + ([] if last else [vm] * 3 + [hbm] * 3),
        out_specs=[vm] * (1 if last else 4),
        scratch_shapes=[
            V((n_p, k_loc, PC), BF16), V((n_f, d_model, PC), BF16), V((n_f, d_model, PC), BF16), V((n_p, f_loc, PC), BF16),
            V((n_p, rows, PC), F32), V((n_p, rows, PC), F32), V((n_p, rows, PC), F32),
            V((rows, d_model), BF16), V((rows, f_loc), BF16), V((rows, k_loc), BF16),
            V((n_p // 2, rows, PC), F32), V((2, rows, PC), F32), V((2, rows, PC), F32), V((rows, PC), F32), V((rows, PC), F32),
            V((heads // 2, rows, hd), F32), V((2, sr // 2, 128), F32),
            V((heads // 4, rows, hd), F32), V((heads // 4, rows, hd), F32), V((2, 2, sr // 4, 128), F32),
            V((heads // 4, rows, hd), F32), V((2, sr // 4, 128), F32),
            dma((n_p,)), dma((n_f,)), dma((n_f,)), dma((n_p,)),
            dma((5,)), dma((5,)), dma((10,)), dma((10,)), dma((14,)), dma((14,)),
        ],
        compiler_params=pltpu.CompilerParams(collective_id=layer, has_side_effects=True, vmem_limit_bytes=VMEM_ALL),
        name=f'block{layer}',
    )(o, sm, sl, u, gain, wo, wg, wu, wd, *nxt)


def solution(mesh):
    sp_size = mesh.shape['sp']

    def local_fn(tok_emb, lengths, key_cache, val_cache, gain_attn, gain_mlp, w_query, w_key, w_value, w_out, w_gate, w_up, w_down):
        n_steps, n_batch, d_model = tok_emb.shape
        n_layers, _, loc_len, kv_loc, hd = key_cache.shape
        rows = n_steps * n_batch
        first_pos = loc_len * sp_size // 2
        table = jnp.asarray(rope_table(first_pos, first_pos, hd))
        u = tok_emb.reshape(rows, d_model)
        kc = key_cache.reshape(n_layers, n_batch, loc_len * kv_loc, hd)
        vc = val_cache.reshape(n_layers, n_batch, loc_len * kv_loc, hd)
        prev = None
        for layer in range(n_layers):
            last = layer == n_layers - 1
            if layer == 0:
                q, k, v, cos_a, sin_a, u = qkv_call(layer, u, gain_attn, table, lengths, w_query, w_key, w_value, n_steps, hd, first_pos)
            nk, nv, o, sm, sl = attn_call(layer, lengths, q, k, v, kc, vc, prev, kv_loc, n_steps, sp_size)
            prev = (nk, nv)
            nxt = () if last else (gain_attn, cos_a, sin_a, w_query, w_key, w_value)
            outs = block_call(layer, last, n_steps, o, sm, sl, u, gain_mlp, w_out, w_gate, w_up, w_down, sp_size, nxt)
            u = outs[0]
            if not last:
                q, k, v = outs[1:]
        return u.reshape(n_steps, n_batch, d_model), prev[0].reshape(key_cache.shape), prev[1].reshape(val_cache.shape)

    cache_spec = P(None, 'dp', 'sp', 'tp', None)
    col_spec = P(None, None, 'tp')
    row_spec = P(None, 'tp', None)
    emb_spec = P(None, 'dp', None)
    return jax.shard_map(local_fn, mesh=mesh, in_specs=(emb_spec, P('dp'), cache_spec, cache_spec, P(), P(), col_spec, col_spec, col_spec, row_spec, col_spec, col_spec, row_spec), out_specs=(emb_spec, cache_spec, cache_spec), check_vma=False)
```

```python
import functools

import jax
import jax.numpy as jnp
import numpy as np
from jax import lax
from jax.experimental import pallas as pl
from jax.experimental.pallas import tpu as pltpu
from jax.sharding import PartitionSpec as P

EPS = 1e-5
ROPE_BASE = 500000.0
F32 = jnp.float32
BF16 = jnp.bfloat16
MESH = pl.DeviceIdType.MESH
PC = 256
VMEM_ALL = 67043328


def rope_table(first_pos, n_pos, head_dim):
    half = head_dim // 2
    inv_freq = (1.0 / (np.float32(ROPE_BASE) ** (np.arange(half).astype(np.float32) * np.float32(2.0 / head_dim)))).astype(np.float32)
    pos = np.arange(first_pos, first_pos + n_pos).astype(np.float32)
    angles = (pos[:, None] * inv_freq[None, :]).astype(np.float32)
    return np.concatenate([np.cos(angles), np.sin(angles)], axis=1).astype(np.float32)


def permutation(rows, n_steps, to_batch_major):
    ri = lax.broadcasted_iota(jnp.int32, (rows, rows), 0)
    ci = lax.broadcasted_iota(jnp.int32, (rows, rows), 1)
    n_batch = rows // n_steps
    if to_batch_major:
        src = (ri % n_steps) * n_batch + ri // n_steps
    else:
        src = (ri % n_batch) * n_steps + ri // n_batch
    return jnp.where(ci == src, 1.0, 0.0).astype(BF16)


def qkv_kernel(layer, n_steps, first_pos, first, *refs):
    if first:
        len_ref, tab_ref, u_ref, gain_ref, wq_ref, wk_ref, wv_ref, q_ref, k_ref, v_ref, cos_ref, sin_ref, up_ref, h_scr = refs
    else:
        u_ref, gain_ref, cos_ref, sin_ref, wq_ref, wk_ref, wv_ref, q_ref, k_ref, v_ref, h_scr = refs
    rows, d_model = u_ref.shape
    hd = cos_ref.shape[1]

    @pl.when(pl.program_id(0) == 0)
    def _():
        x = u_ref[...].astype(F32)
        inv = lax.rsqrt(jnp.sum(x * x, axis=-1, keepdims=True) * (1.0 / d_model) + EPS)
        h = (x * inv * gain_ref[layer:layer + 1, :].astype(F32)).astype(BF16)
        if first:
            perm = permutation(rows, n_steps, True)
            h_scr[...] = jnp.dot(perm, h, preferred_element_type=F32).astype(BF16)
            up_ref[...] = jnp.dot(perm, u_ref[...], preferred_element_type=F32).astype(BF16)
            for b in range(rows // n_steps):
                cos_ref[b * n_steps:(b + 1) * n_steps, :] = tab_ref[pl.ds(len_ref[b] - first_pos, n_steps), :]
            both = cos_ref[...]
            swap = pltpu.roll(both, hd // 2, 1)
            low = lax.broadcasted_iota(jnp.int32, both.shape, 1) < hd // 2
            cos_ref[...] = jnp.where(low, both, swap)
            sin_ref[...] = jnp.where(low, -swap, both)
        else:
            h_scr[...] = h

    h = h_scr[...]
    cos_a, sin_a = cos_ref[...], sin_ref[...]

    def rot(x):
        return (x * cos_a + pltpu.roll(x, hd // 2, 1) * sin_a).astype(BF16).astype(F32)

    q = jnp.dot(h, wq_ref[0], preferred_element_type=F32)
    for j in range(q_ref.shape[0]):
        q_ref[j] = rot(q[:, j * hd:(j + 1) * hd])
    k = jnp.dot(h, wk_ref[0], preferred_element_type=F32)
    k_ref[0] = rot(k)
    v = jnp.dot(h, wv_ref[0], preferred_element_type=F32)
    v_ref[0] = v.astype(BF16).astype(F32)


def qkv_call(layer, u, gain, rope, lengths, wq, wk, wv, n_steps, hd, first_pos):
    rows, d_model = u.shape
    kv_loc = wk.shape[2] // hd
    heads = wq.shape[2] // hd
    grp = heads // kv_loc
    first = layer == 0
    full = lambda shape: pl.BlockSpec(shape, lambda j: (0,) * len(shape))
    weights = [
        pl.BlockSpec((1, d_model, grp * hd), lambda j: (layer, 0, j)),
        pl.BlockSpec((1, d_model, hd), lambda j: (layer, 0, j)),
        pl.BlockSpec((1, d_model, hd), lambda j: (layer, 0, j)),
    ]
    out_specs = [
        pl.BlockSpec((grp, rows, hd), lambda j: (j, 0, 0)),
        pl.BlockSpec((1, rows, hd), lambda j: (j, 0, 0)),
        pl.BlockSpec((1, rows, hd), lambda j: (j, 0, 0)),
    ]
    out_shape = [
        jax.ShapeDtypeStruct((heads, rows, hd), F32),
        jax.ShapeDtypeStruct((kv_loc, rows, hd), F32),
        jax.ShapeDtypeStruct((kv_loc, rows, hd), F32),
    ]
    if first:
        args = [lengths, rope, u, gain, wq, wk, wv]
        in_specs = [pl.BlockSpec(memory_space=pltpu.SMEM), full(rope.shape), full(u.shape), full(gain.shape)] + weights
        out_specs += [full((rows, hd)), full((rows, hd)), full((rows, d_model))]
        out_shape += [jax.ShapeDtypeStruct((rows, hd), F32)] * 2 + [jax.ShapeDtypeStruct((rows, d_model), BF16)]
    else:
        args = [u, gain, *rope, wq, wk, wv]
        in_specs = [full(u.shape), full(gain.shape), full((rows, hd)), full((rows, hd))] + weights
    return pl.pallas_call(
        functools.partial(qkv_kernel, layer, n_steps, first_pos, first),
        grid=(kv_loc,),
        in_specs=in_specs,
        out_specs=out_specs,
        out_shape=out_shape,
        scratch_shapes=[pltpu.VMEM((rows, d_model), BF16)],
        compiler_params=pltpu.CompilerParams(vmem_limit_bytes=VMEM_ALL),
        name=f'qkv{layer}',
    )(*args)


SEQS = 4
SLOTS = 8
AHEAD = 8


def attn_kernel(layer, n_kv, n_steps, sp_size, has_prev, len_ref, q_ref, kn_ref, vn_ref, k_hbm, v_hbm, *rest):
    if has_prev:
        rest = rest[2:]
    ko_hbm, vo_hbm, o_ref, sm_ref, sl_ref, code, kb, vb, in_sem, out_sem = rest
    my_sp = lax.axis_index('sp').astype(jnp.int32)
    heads, all_rows, hd = q_ref.shape
    n_batch = all_rows // n_steps
    n_iter = n_batch // SEQS
    r8 = 2 * n_steps
    rows = heads * r8
    n_cols = kb.shape[2]
    row_kv = rows // n_kv

    def reads(i):
        slot = lax.rem(i, SLOTS)
        src = pl.ds(i * SEQS, SEQS)
        return (pltpu.make_async_copy(k_hbm.at[layer, src], kb.at[slot], in_sem.at[slot, 0]),
                pltpu.make_async_copy(v_hbm.at[layer, src], vb.at[slot], in_sem.at[slot, 1]))

    def writes(i):
        slot = lax.rem(i, SLOTS)
        dst = pl.ds(i * SEQS, SEQS)
        return (pltpu.make_async_copy(kb.at[slot], ko_hbm.at[layer, dst], out_sem.at[slot, 0]),
                pltpu.make_async_copy(vb.at[slot], vo_hbm.at[layer, dst], out_sem.at[slot, 1]))

    for i in range(min(AHEAD, n_iter)):
        for cp in reads(i):
            cp.start()

    ri = lax.broadcasted_iota(jnp.int32, (rows, n_cols), 0)
    ci = lax.broadcasted_iota(jnp.int32, (rows, n_cols), 1)
    same = (ci % n_kv) == (ri // row_kv)
    code[...] = jnp.where(same, (ci // n_kv) * sp_size + my_sp, 2**30)
    sm_ref[...] = jnp.zeros_like(sm_ref)
    sl_ref[...] = jnp.zeros_like(sl_ref)
    rcol = lax.broadcasted_iota(jnp.int32, (rows, 1), 0) % r8
    first = rcol < n_steps
    row16 = lax.broadcasted_iota(jnp.int32, (16, hd), 0)
    lane = lax.broadcasted_iota(jnp.int32, sm_ref.shape, 1)
    per = 16 // n_kv

    def body(i, _):
        slot_b = lax.rem(i, SLOTS)
        for cp in reads(i):
            cp.wait()
        for b in range(SEQS):
            seq = i * SEQS + b
            length = len_ref[seq]
            step = lax.rem(my_sp - lax.rem(length, sp_size) + sp_size, sp_size)
            slot = lax.div(length + step, sp_size)
            base = pl.multiple_of(lax.div(slot, per) * 16, 16)
            mine = row16 // n_kv == lax.rem(slot, per)
            new_row = seq * n_steps + step
            for buf, src in ((kb, kn_ref), (vb, vn_ref)):
                fresh = jnp.broadcast_to(src[0, pl.ds(new_row, 1), :], (16, hd))
                for j in range(1, n_kv):
                    fresh = jnp.where(row16 % n_kv == j, jnp.broadcast_to(src[j, pl.ds(new_row, 1), :], (16, hd)), fresh)
                old = buf[slot_b, b, pl.ds(base, 16), :]
                buf[slot_b, b, pl.ds(base, 16), :] = jnp.where(mine, fresh, old.astype(F32)).astype(BF16)
        for cp in writes(i):
            cp.start()
        sm, sl = sm_ref[...], sl_ref[...]
        for t in range(SEQS // 2):
            pair = i * (SEQS // 2) + t
            r0 = pl.multiple_of(pair * r8, r8)
            q = q_ref[:, pl.ds(r0, r8), :].reshape(rows, hd)
            limit = jnp.where(first, len_ref[2 * pair], len_ref[2 * pair + 1]) + rcol % n_steps
            zero = jnp.zeros_like(q)
            q2 = jnp.concatenate([jnp.where(first, q, zero), jnp.where(first, zero, q)], axis=1).astype(BF16)
            k2 = jnp.concatenate([kb[slot_b, 2 * t], kb[slot_b, 2 * t + 1]], axis=1)
            s = lax.dot_general(q2, k2, (((1,), (1,)), ((), ())), preferred_element_type=F32)
            s = jnp.where(code[...] <= limit, s * hd ** -0.5, -1e30)
            m = jnp.max(s, axis=-1, keepdims=True)
            p = jnp.exp(s - m)
            l = jnp.sum(p, axis=-1, keepdims=True)
            v2 = jnp.concatenate([vb[slot_b, 2 * t], vb[slot_b, 2 * t + 1]], axis=1)
            o = jnp.dot(p.astype(BF16), v2, preferred_element_type=F32)
            o = jnp.where(first, o[:, :hd], o[:, hd:])
            o_ref[:, pl.ds(r0, r8), :] = o.reshape(heads, r8, hd)
            sm = jnp.where(lane == pair, m, sm)
            sl = jnp.where(lane == pair, l, sl)
        sm_ref[...] = sm
        sl_ref[...] = sl

        if AHEAD < n_iter:
            @pl.when(jnp.logical_and(i + AHEAD >= SLOTS, i + AHEAD < n_iter))
            def _():
                for cp in writes(i + AHEAD - SLOTS):
                    cp.wait()

            @pl.when(i + AHEAD < n_iter)
            def _():
                for cp in reads(i + AHEAD):
                    cp.start()
        return 0

    lax.fori_loop(0, n_iter, body, 0)
    for i in range(max(0, n_iter - SLOTS), n_iter):
        for cp in writes(i):
            cp.wait()


def attn_call(layer, lengths, q, kn, vn, kc, vc, prev, n_kv, n_steps, sp_size):
    n_layers, n_batch, n_cols, hd = kc.shape
    heads, rows, _ = q.shape
    srows = heads * 2 * n_steps
    vm = pl.BlockSpec(memory_space=pltpu.VMEM)
    hbm = pl.BlockSpec(memory_space=pl.ANY)
    in_specs = [pl.BlockSpec(memory_space=pltpu.SMEM), vm, vm, vm, hbm, hbm]
    args = [lengths, q, kn, vn, kc, vc]
    aliases = {}
    if prev is not None:
        in_specs += [hbm, hbm]
        args += list(prev)
        aliases = {6: 0, 7: 1}
    return pl.pallas_call(
        functools.partial(attn_kernel, layer, n_kv, n_steps, sp_size, prev is not None),
        in_specs=in_specs,
        out_specs=[hbm, hbm, vm, vm, vm],
        out_shape=[
            jax.ShapeDtypeStruct(kc.shape, kc.dtype), jax.ShapeDtypeStruct(vc.shape, vc.dtype),
            jax.ShapeDtypeStruct((heads, rows, hd), F32),
            jax.ShapeDtypeStruct((srows, 128), F32), jax.ShapeDtypeStruct((srows, 128), F32),
        ],
        scratch_shapes=[
            pltpu.VMEM((srows, n_cols), jnp.int32),
            pltpu.VMEM((SLOTS, SEQS, n_cols, hd), BF16), pltpu.VMEM((SLOTS, SEQS, n_cols, hd), BF16),
            pltpu.SemaphoreType.DMA((SLOTS, 2)), pltpu.SemaphoreType.DMA((SLOTS, 2)),
        ],
        input_output_aliases=aliases,
        compiler_params=pltpu.CompilerParams(vmem_limit_bytes=VMEM_ALL),
        name=f'attn{layer}',
    )(*args)


def block_kernel(layer, last, n_steps, o_hbm, sm_hbm, sl_hbm, u_hbm, gain_ref, wo_hbm, wg_hbm, wu_hbm, wd_hbm, *refs):
    has_next = not last
    if has_next:
        gain_a_ref, cos_ref, sin_ref, wq_hbm, wk_hbm, wv_hbm, out_ref, q_ref, k_ref, v_ref, *refs = refs
    else:
        out_ref, *refs = refs
    block_body(layer, last, n_steps, has_next, o_hbm, sm_hbm, sl_hbm, u_hbm, gain_ref, wo_hbm, wg_hbm, wu_hbm, wd_hbm,
               (gain_a_ref, cos_ref, sin_ref, wq_hbm, wk_hbm, wv_hbm) if has_next else None, out_ref,
               (q_ref, k_ref, v_ref) if has_next else None, *refs)


def block_body(layer, last, n_steps, has_next, o_hbm, sm_hbm, sl_hbm, u_hbm, gain_ref, wo_hbm, wg_hbm, wu_hbm, wd_hbm, nxt, out_ref, qkv,
                 o_ref, sm_ref, sl_ref, u_ref, in_sem, wo_v, wg_v, wu_v, wd_v, part, g1, g2, h2, act, att,
                 r_d, r_x1, r_y1, r_x2, r_y2, r_o, r_st, mo_s, mo_k, mst, r_o2, r_st2,
                 wo_sem, wg_sem, wu_sem, wd_sem, m_send, m_recv, rs_send, rs_recv, ag_send, ag_recv):
    if has_next:
        gain_a_ref, cos_ref, sin_ref, wq_hbm, wk_hbm, wv_hbm = nxt
        q_ref, k_ref, v_ref = qkv
    sp = lax.axis_index('sp')
    y = lax.axis_index('tp')
    c = lax.rem(sp, 2)
    x = lax.div(sp, 2)
    rows = u_ref.shape[0]
    d_model = u_ref.shape[1]
    hd = o_ref.shape[2]
    heads = o_ref.shape[0]
    n_pieces = d_model // PC
    f_loc = wd_v.shape[1]
    k_loc = wo_v.shape[1]
    n_f = wg_v.shape[0]
    core_dev = {'sp': 2 * x + 1 - c}
    x_dev = {'sp': 2 * (1 - x) + c}
    y_dev = {'tp': 1 - y}

    def piece(half, kind, far, sub):
        return half * 8 + kind * 4 + far * 2 + sub

    order = []
    for far_x, far_y in ((1 - x, 1 - y), (x, y)):
        for half in (1 - c, c):
            for kind, far in ((0, far_x), (1, far_y)):
                for sub in ((1 - y, y) if kind == 0 else (1 - x, x)):
                    order.append(piece(half, kind, far, sub))

    in_copies = {}
    half_rows = rows // 2
    half_of = [pl.ds(r * half_rows, half_rows) for r in range(2)]
    for n, (key, src, dst) in enumerate((
            ('m', sm_hbm, sm_ref), ('l', sl_hbm, sl_ref), (0, o_hbm.at[:, half_of[0]], o_ref.at[:, half_of[0]]),
            (1, o_hbm.at[:, half_of[1]], o_ref.at[:, half_of[1]]), ('u', u_hbm, u_ref))):
        in_copies[key] = pltpu.make_async_copy(src, dst, in_sem.at[n])
        in_copies[key].start()
    copies = {}

    def start(key, src, dst, sem):
        cp = pltpu.make_async_copy(src, dst, sem)
        cp.start()
        copies[key] = cp

    rem_row = pl.multiple_of((8 * c + 4 * x) * hd, hd)
    for i in range(n_pieces):
        start(('o', i), wo_hbm.at[layer, pl.ds(rem_row, k_loc), pl.ds(pl.multiple_of(order[i] * PC, PC), PC)],
              wo_v.at[i // 2, :, (i % 2) * PC:(i % 2 + 1) * PC], wo_sem.at[i])

    barrier = pltpu.get_barrier_semaphore()
    for dev in (core_dev, x_dev, y_dev):
        pl.semaphore_signal(barrier, inc=1, device_id=dev, device_id_type=MESH)
    pl.semaphore_wait(barrier, 3)

    def remote(src, dst, send, recv, dev):
        cp = pltpu.make_async_remote_copy(src_ref=src, dst_ref=dst, send_sem=send, recv_sem=recv, device_id=dev, device_id_type=MESH)
        cp.start()
        return cp

    hh = heads // 2
    hq = heads // 4
    sr = sm_ref.shape[0]
    away = 1 - c
    away_rows = pl.ds(pl.multiple_of(away * (sr // 2), 8), sr // 2)
    in_copies['m'].wait()
    in_copies['l'].wait()
    d_st = [remote(sm_ref.at[away_rows], r_st.at[0], m_send.at[0], m_recv.at[0], core_dev),
            remote(sl_ref.at[away_rows], r_st.at[1], m_send.at[1], m_recv.at[1], core_dev)]
    d_o = []
    for r in range(2):
        in_copies[r].wait()
        d_o.append(remote(o_ref.at[pl.ds(away * hh, hh), half_of[r]], r_o.at[:, half_of[r]], m_send.at[2 + r], m_recv.at[2 + r], core_dev))
    pending = d_st + d_o

    f_off = pl.multiple_of(sp * f_loc, PC)
    def gate_copy(i):
        col = pl.ds(pl.multiple_of(f_off + i * PC, PC), PC)
        return (pltpu.make_async_copy(wg_hbm.at[layer, :, col], wg_v.at[i], wg_sem.at[i]),
                pltpu.make_async_copy(wu_hbm.at[layer, :, col], wu_v.at[i], wu_sem.at[i]))

    for i in range(n_f):
        for cp in gate_copy(i):
            cp.start()
    for i in range(n_pieces):
        start(('d', i), wd_hbm.at[layer, pl.ds(f_off, f_loc), pl.ds(pl.multiple_of(order[i] * PC, PC), PC)],
              wd_v.at[i // 2, :, (i % 2) * PC:(i % 2 + 1) * PC], wd_sem.at[i])

    def merge_into(r, dst, st_dst, src_o, m1, l1, src_o2, m2, l2, n_heads):
        mx = jnp.maximum(m1, m2)
        f1 = jnp.exp(m1 - mx)
        f2 = jnp.exp(m2 - mx)
        ln = l1 * f1 + l2 * f2
        st_dst(mx, ln)
        for h in range(n_heads):
            for t in range(r * half_rows // 8, (r + 1) * half_rows // 8):
                a = jnp.broadcast_to(f1[8 * h:8 * h + 8, t:t + 1], (8, hd))
                b = jnp.broadcast_to(f2[8 * h:8 * h + 8, t:t + 1], (8, hd))
                dst(h, t, src_o(h, t) * a + src_o2(h, t) * b, ln)

    def core_merge(r, q4, dst_o, slot):
        lo = pl.multiple_of(c * (sr // 2) + q4 * (sr // 4), 8)
        lr = pl.multiple_of(q4 * (sr // 4), 8)
        n = sr // 4

        def st_dst(mx, ln):
            if r == 0:
                mst[slot, 0] = mx
                mst[slot, 1] = ln

        def dst(h, t, val, ln):
            dst_o[h, 8 * t:8 * t + 8, :] = val

        merge_into(r, dst, st_dst,
                   lambda h, t: o_ref[c * hh + q4 * hq + h, 8 * t:8 * t + 8, :], sm_ref[pl.ds(lo, n)], sl_ref[pl.ds(lo, n)],
                   lambda h, t: r_o[q4 * hq + h, 8 * t:8 * t + 8, :], r_st[0, pl.ds(lr, n)], r_st[1, pl.ds(lr, n)], hq)

    x_st = []

    def merge_chain(r):
        if r == 0:
            for cp in d_st:
                cp.wait_recv()
        d_o[r].wait_recv()
        core_merge(r, 1 - x, mo_s, 0)
        if r == 0:
            x_st.append(remote(mst.at[0], r_st2, m_send.at[4], m_recv.at[4], x_dev))
            pending.append(x_st[0])
        x_o = remote(mo_s.at[:, half_of[r]], r_o2.at[:, half_of[r]], m_send.at[5 + r], m_recv.at[5 + r], x_dev)
        pending.append(x_o)
        core_merge(r, x, mo_k, 1)
        yield
        if r == 0:
            x_st[0].wait_recv()
        x_o.wait_recv()

        def fin(h, t, val, ln):
            den = jnp.broadcast_to(ln[8 * h:8 * h + 8, t:t + 1], (8, hd))
            mo_k[h, 8 * t:8 * t + 8, :] = val / den

        merge_into(r, fin, lambda mx, ln: None,
                   lambda h, t: mo_k[h, 8 * t:8 * t + 8, :], mst[1, 0], mst[1, 1],
                   lambda h, t: r_o2[h, 8 * t:8 * t + 8, :], r_st2[0], r_st2[1], hq)
        for h in range(hq):
            att[half_of[r], h * hd:(h + 1) * hd] = mo_k[h, half_of[r]].astype(BF16)

    def rs(r, n, src, dst, dev):
        cp = remote(src, dst, rs_send.at[10 * r + n], rs_recv.at[10 * r + n], dev)
        pending.append(cp)
        return cp

    def sum_front(halves, product):
        r0 = halves[0]
        R = pl.ds(r0 * half_rows, len(halves) * half_rows)
        link = {r: [None] * 4 for r in halves}

        def core_part(first, at):
            out = []
            for k in range(2):
                i = first + 2 * k
                val = product(i // 2, R, r0 == 0)
                part[i, R] = val[:, :PC]
                part[i + 1, R] = val[:, PC:]
                out.append(rs(r0, at // 2 + k, part.at[pl.ds(i, 2), R], r_d.at[pl.ds(at + 2 * k, 2), R], core_dev))
            return out

        def own_part(first, at, k, d_in):
            i = first + 2 * k
            val = product(i // 2, R, r0 == 0)
            d_in[k].wait_recv()
            part[i, R] = val[:, :PC] + r_d[at + 2 * k, R]
            part[i + 1, R] = val[:, PC:] + r_d[at + 2 * k + 1, R]

        d_in = core_part(0, 0)
        for k, (buf, dev) in enumerate(((r_x1, x_dev), (r_y1, y_dev))):
            own_part(4, 0, k, d_in)
            for r in halves:
                for j in range(2):
                    link[r][2 * k + j] = rs(r, 4 + 2 * k + j, part.at[4 + 2 * k + j, half_of[r]], buf.at[j, half_of[r]], dev)
        d_in = core_part(8, 4)
        for k in range(2):
            own_part(12, 4, k, d_in)
        return link

    def sum_back(r, link, resid, g):
        R = half_of[r]

        def ag(n, p, dev):
            cp = remote(g.at[p, R], g.at[p, R], ag_send.at[14 * r + n], ag_recv.at[14 * r + n], dev)
            pending.append(cp)
            return cp

        link[0].wait_recv()
        part[12, R] = part[12, R] + r_x1[0, R]
        a2 = rs(r, 8, part.at[12, R], r_y2.at[R], y_dev)
        link[2].wait_recv()
        part[14, R] = part[14, R] + r_y1[0, R]
        b2 = rs(r, 9, part.at[14, R], r_x2.at[R], x_dev)
        link[1].wait_recv()
        part[13, R] = part[13, R] + r_x1[1, R]
        link[3].wait_recv()
        part[15, R] = part[15, R] + r_y1[1, R]
        yield
        pa = piece(c, 0, x, y)
        pb = piece(c, 1, y, x)
        a2.wait_recv()
        g[pa, R] = (resid(pa, R) + (part[13, R] + r_y2[R])).astype(BF16).astype(F32)
        ya = ag(0, pa, y_dev)
        b2.wait_recv()
        g[pb, R] = (resid(pb, R) + (part[15, R] + r_x2[R])).astype(BF16).astype(F32)
        xb = ag(3, pb, x_dev)
        xa = ag(1, pa, x_dev)
        yb = ag(4, pb, y_dev)
        last_in = [ag(2, pa, core_dev), ag(5, pb, core_dev)]
        yield
        ya.wait_recv()
        p = piece(c, 0, x, 1 - y)
        xf = ag(6, p, x_dev)
        last_in.append(ag(7, p, core_dev))
        xb.wait_recv()
        p = piece(c, 1, y, 1 - x)
        yf = ag(8, p, y_dev)
        last_in.append(ag(9, p, core_dev))
        yield
        xa.wait_recv()
        last_in.append(ag(10, piece(c, 0, 1 - x, y), core_dev))
        yb.wait_recv()
        last_in.append(ag(11, piece(c, 1, 1 - y, x), core_dev))
        xf.wait_recv()
        last_in.append(ag(12, piece(c, 0, 1 - x, 1 - y), core_dev))
        yf.wait_recv()
        last_in.append(ag(13, piece(c, 1, 1 - y, 1 - x), core_dev))
        yield
        for cp in last_in:
            cp.wait_recv()

    def interleave(chains):
        chains = list(chains)
        while chains:
            for ch in list(chains):
                if next(ch, 'end') == 'end':
                    chains.remove(ch)
        for cp in pending:
            cp.wait_send()
        pending.clear()

    def out_product(k, R, fetch):
        if fetch:
            copies[('o', 2 * k)].wait()
            copies[('o', 2 * k + 1)].wait()
        return jnp.dot(att[R], wo_v[k], preferred_element_type=F32)

    def u_resid(p, R):
        return u_ref[R, pl.ds(pl.multiple_of(p * PC, PC), PC)].astype(F32)

    def first_part(r):
        yield from merge_chain(r)
        link = sum_front([r], out_product)
        yield
        if r == 0:
            in_copies['u'].wait()
        yield from sum_back(r, link[r], u_resid, g1)

    interleave(first_part(r) for r in range(2))

    def norm(g, gains, row):
        sq = jnp.zeros((rows, PC), F32)
        for i in range(n_pieces):
            sq = sq + g[i] * g[i]
        inv = lax.rsqrt(jnp.sum(sq, axis=-1, keepdims=True) * (1.0 / d_model) + EPS)
        for i in range(n_pieces):
            cols = slice(i * PC, (i + 1) * PC)
            h2[:, cols] = (g[i] * inv * gains[row:row + 1, cols].astype(F32)).astype(BF16)

    norm(g1, gain_ref, layer)

    def gate_up(i, _):
        cg, cu = gate_copy(i)
        cg.wait()
        ga = jnp.dot(h2[...], wg_v[i], preferred_element_type=F32)
        cu.wait()
        up = jnp.dot(h2[...], wu_v[i], preferred_element_type=F32)
        act[:, pl.ds(pl.multiple_of(i * PC, PC), PC)] = (ga * jax.nn.sigmoid(ga) * up).astype(BF16)
        return 0

    lax.fori_loop(0, n_f, gate_up, 0)

    n_q = q_ref.shape[0] * hd // (2 * PC) if has_next else 0

    def next_copy(j):
        out = []
        for t, (buf, sem) in enumerate(((wg_v, wg_sem), (wu_v, wu_sem))):
            if isinstance(j, int) and j >= n_q:
                src = (wk_hbm, wv_hbm)[j - n_q].at[layer + 1, :, t * PC:(t + 1) * PC]
            else:
                src = wq_hbm.at[layer + 1, :, pl.ds(pl.multiple_of((2 * j + t) * PC, PC), PC)]
            out.append(pltpu.make_async_copy(src, buf.at[j], sem.at[j]))
        return out

    if has_next:
        for j in range(n_q + 2):
            for cp in next_copy(j):
                cp.start()

    def down_product(k, R, fetch):
        copies[('d', 2 * k)].wait()
        copies[('d', 2 * k + 1)].wait()
        return jnp.dot(act[...], wd_v[k], preferred_element_type=F32)

    links = sum_front([0, 1], down_product)
    interleave(sum_back(r, links[r], lambda p, R: g1[p, R], g2) for r in range(2))
    back = permutation(rows, n_steps, False) if last else None
    for i in range(n_pieces):
        val = g2[i].astype(BF16)
        if last:
            val = jnp.dot(back, val, preferred_element_type=F32).astype(BF16)
        out_ref[:, i * PC:(i + 1) * PC] = val

    if has_next:
        norm(g2, gain_a_ref, layer + 1)
        cos_a, sin_a = cos_ref[...], sin_ref[...]

        def rot(z):
            return (z * cos_a + pltpu.roll(z, hd // 2, 1) * sin_a).astype(BF16).astype(F32)

        def heads_of(j, store):
            for t, (buf, cp) in enumerate(zip((wg_v, wu_v), next_copy(j))):
                cp.wait()
                val = jnp.dot(h2[...], buf[j], preferred_element_type=F32)
                for e in range(PC // hd):
                    store(t * (PC // hd) + e, val[:, e * hd:(e + 1) * hd])

        def q_pair(j, _):
            def store(e, val):
                q_ref[2 * (PC // hd) * j + e] = rot(val)
            heads_of(j, store)
            return 0

        def store_k(e, val):
            k_ref[e] = rot(val)

        def store_v(e, val):
            v_ref[e] = val.astype(BF16).astype(F32)

        lax.fori_loop(0, n_q, q_pair, 0)
        heads_of(n_q, store_k)
        heads_of(n_q + 1, store_v)


def block_call(layer, last, n_steps, o, sm, sl, u, gain, wo, wg, wu, wd, sp_size, nxt):
    rows, d_model = u.shape
    heads, _, hd = o.shape
    n_p = d_model // PC
    k_loc = wo.shape[1] // sp_size
    f_loc = wd.shape[1] // sp_size
    n_f = f_loc // PC
    sr = sm.shape[0]
    V = pltpu.VMEM
    dma = pltpu.SemaphoreType.DMA
    vm = pl.BlockSpec(memory_space=pltpu.VMEM)
    hbm = pl.BlockSpec(memory_space=pl.ANY)
    return pl.pallas_call(
        functools.partial(block_kernel, layer, last, n_steps),
        out_shape=[jax.ShapeDtypeStruct((rows, d_model), BF16)] + ([] if last else [
            jax.ShapeDtypeStruct((heads, rows, hd), F32),
            jax.ShapeDtypeStruct((nxt[4].shape[2] // hd, rows, hd), F32),
            jax.ShapeDtypeStruct((nxt[4].shape[2] // hd, rows, hd), F32)]),
        in_specs=[hbm] * 4 + [vm] + [hbm] * 4 + ([] if last else [vm] * 3 + [hbm] * 3),
        out_specs=[vm] * (1 if last else 4),
        scratch_shapes=[
            V(o.shape, F32), V(sm.shape, F32), V(sl.shape, F32), V(u.shape, BF16), dma((5,)),
            V((n_p // 2, k_loc, 2 * PC), BF16), V((n_f, d_model, PC), BF16), V((n_f, d_model, PC), BF16), V((n_p // 2, f_loc, 2 * PC), BF16),
            V((n_p, rows, PC), F32), V((n_p, rows, PC), F32), V((n_p, rows, PC), F32),
            V((rows, d_model), BF16), V((rows, f_loc), BF16), V((rows, k_loc), BF16),
            V((n_p // 2, rows, PC), F32), V((2, rows, PC), F32), V((2, rows, PC), F32), V((rows, PC), F32), V((rows, PC), F32),
            V((heads // 2, rows, hd), F32), V((2, sr // 2, 128), F32),
            V((heads // 4, rows, hd), F32), V((heads // 4, rows, hd), F32), V((2, 2, sr // 4, 128), F32),
            V((heads // 4, rows, hd), F32), V((2, sr // 4, 128), F32),
            dma((n_p,)), dma((n_f,)), dma((n_f,)), dma((n_p,)),
            dma((7,)), dma((7,)), dma((20,)), dma((20,)), dma((28,)), dma((28,)),
        ],
        compiler_params=pltpu.CompilerParams(collective_id=layer, has_side_effects=True, vmem_limit_bytes=VMEM_ALL),
        name=f'block{layer}',
    )(o, sm, sl, u, gain, wo, wg, wu, wd, *nxt)


def solution(mesh):
    sp_size = mesh.shape['sp']

    def local_fn(tok_emb, lengths, key_cache, val_cache, gain_attn, gain_mlp, w_query, w_key, w_value, w_out, w_gate, w_up, w_down):
        n_steps, n_batch, d_model = tok_emb.shape
        n_layers, _, loc_len, kv_loc, hd = key_cache.shape
        rows = n_steps * n_batch
        first_pos = loc_len * sp_size // 2
        table = jnp.asarray(rope_table(first_pos, first_pos, hd))
        u = tok_emb.reshape(rows, d_model)
        kc = key_cache.reshape(n_layers, n_batch, loc_len * kv_loc, hd)
        vc = val_cache.reshape(n_layers, n_batch, loc_len * kv_loc, hd)
        prev = None
        for layer in range(n_layers):
            last = layer == n_layers - 1
            if layer == 0:
                q, k, v, cos_a, sin_a, u = qkv_call(layer, u, gain_attn, table, lengths, w_query, w_key, w_value, n_steps, hd, first_pos)
            nk, nv, o, sm, sl = attn_call(layer, lengths, q, k, v, kc, vc, prev, kv_loc, n_steps, sp_size)
            prev = (nk, nv)
            nxt = () if last else (gain_attn, cos_a, sin_a, w_query, w_key, w_value)
            outs = block_call(layer, last, n_steps, o, sm, sl, u, gain_mlp, w_out, w_gate, w_up, w_down, sp_size, nxt)
            u = outs[0]
            if not last:
                q, k, v = outs[1:]
        return u.reshape(n_steps, n_batch, d_model), prev[0].reshape(key_cache.shape), prev[1].reshape(val_cache.shape)

    cache_spec = P(None, 'dp', 'sp', 'tp', None)
    col_spec = P(None, None, 'tp')
    row_spec = P(None, 'tp', None)
    emb_spec = P(None, 'dp', None)
    return jax.shard_map(local_fn, mesh=mesh, in_specs=(emb_spec, P('dp'), cache_spec, cache_spec, P(), P(), col_spec, col_spec, col_spec, row_spec, col_spec, col_spec, row_spec), out_specs=(emb_spec, cache_spec, cache_spec), check_vma=False)
```

```python
import functools

import jax
import jax.numpy as jnp
import numpy as np
from jax import lax
from jax.experimental import pallas as pl
from jax.experimental.pallas import tpu as pltpu
from jax.sharding import PartitionSpec as P

EPS = 1e-5
ROPE_BASE = 500000.0
F32 = jnp.float32
BF16 = jnp.bfloat16
MESH = pl.DeviceIdType.MESH
PC = 256
VMEM_ALL = 67043328


def rope_table(first_pos, n_pos, head_dim):
    half = head_dim // 2
    inv_freq = (1.0 / (np.float32(ROPE_BASE) ** (np.arange(half).astype(np.float32) * np.float32(2.0 / head_dim)))).astype(np.float32)
    pos = np.arange(first_pos, first_pos + n_pos).astype(np.float32)
    angles = (pos[:, None] * inv_freq[None, :]).astype(np.float32)
    return np.concatenate([np.cos(angles), np.sin(angles)], axis=1).astype(np.float32)


def permutation(rows, n_steps, to_batch_major):
    ri = lax.broadcasted_iota(jnp.int32, (rows, rows), 0)
    ci = lax.broadcasted_iota(jnp.int32, (rows, rows), 1)
    n_batch = rows // n_steps
    if to_batch_major:
        src = (ri % n_steps) * n_batch + ri // n_steps
    else:
        src = (ri % n_batch) * n_steps + ri // n_batch
    return jnp.where(ci == src, 1.0, 0.0).astype(BF16)


SEQS = 4
SLOTS = 8
AHEAD = 8


def attn_kernel(layer, n_kv, n_steps, sp_size, len_ref, q_ref, kn_ref, vn_ref, k_hbm, v_hbm, _k, _v, *rest):
    ko_hbm, vo_hbm, o_ref, sm_ref, sl_ref, code, kb, vb, in_sem, out_sem = rest
    attn_body(layer, n_kv, n_steps, sp_size, lambda: None, len_ref, q_ref, kn_ref, vn_ref, k_hbm, v_hbm,
              ko_hbm, vo_hbm, o_ref, sm_ref, sl_ref, code, kb, vb, in_sem, out_sem)


def first_kernel(n_kv, n_steps, sp_size, first_pos, len_ref, tab_ref, u_ref, gain_ref, wq_hbm, wk_hbm, wv_hbm, k_hbm, v_hbm,
                 ko_hbm, vo_hbm, o_ref, sm_ref, sl_ref, cos_ref, sin_ref, up_ref,
                 q_s, k_s, v_s, h_scr, wq_v, wk_v, wv_v, w_sem, code, kb, vb, in_sem, out_sem):
    rows, d_model = u_ref.shape
    hd = cos_ref.shape[1]
    n_q, _, cols = wq_v.shape
    fetch = [pltpu.make_async_copy(wq_hbm.at[0, :, j * cols:(j + 1) * cols], wq_v.at[j], w_sem.at[j]) for j in range(n_q)]
    fetch.append(pltpu.make_async_copy(wk_hbm.at[0], wk_v, w_sem.at[n_q]))
    fetch.append(pltpu.make_async_copy(wv_hbm.at[0], wv_v, w_sem.at[n_q + 1]))
    for cp in fetch:
        cp.start()

    def qkv():
        x = u_ref[...].astype(F32)
        inv = lax.rsqrt(jnp.sum(x * x, axis=-1, keepdims=True) * (1.0 / d_model) + EPS)
        h = (x * inv * gain_ref[0:1, :].astype(F32)).astype(BF16)
        perm = permutation(rows, n_steps, True)
        h_scr[...] = jnp.dot(perm, h, preferred_element_type=F32).astype(BF16)
        up_ref[...] = jnp.dot(perm, u_ref[...], preferred_element_type=F32).astype(BF16)
        for b in range(rows // n_steps):
            cos_ref[b * n_steps:(b + 1) * n_steps, :] = tab_ref[pl.ds(len_ref[b] - first_pos, n_steps), :]
        both = cos_ref[...]
        swap = pltpu.roll(both, hd // 2, 1)
        low = lax.broadcasted_iota(jnp.int32, both.shape, 1) < hd // 2
        cos_a = jnp.where(low, both, swap)
        sin_a = jnp.where(low, -swap, both)
        cos_ref[...] = cos_a
        sin_ref[...] = sin_a

        def rot(z):
            return (z * cos_a + pltpu.roll(z, hd // 2, 1) * sin_a).astype(BF16).astype(F32)

        per = cols // hd
        for j in range(n_q):
            fetch[j].wait()
            q = jnp.dot(h_scr[...], wq_v[j], preferred_element_type=F32)
            for e in range(per):
                q_s[j * per + e] = rot(q[:, e * hd:(e + 1) * hd])
        fetch[n_q].wait()
        k = jnp.dot(h_scr[...], wk_v[...], preferred_element_type=F32)
        for e in range(n_kv):
            k_s[e] = rot(k[:, e * hd:(e + 1) * hd])
        fetch[n_q + 1].wait()
        v = jnp.dot(h_scr[...], wv_v[...], preferred_element_type=F32)
        for e in range(n_kv):
            v_s[e] = v[:, e * hd:(e + 1) * hd].astype(BF16).astype(F32)

    attn_body(0, n_kv, n_steps, sp_size, qkv, len_ref, q_s, k_s, v_s, k_hbm, v_hbm,
              ko_hbm, vo_hbm, o_ref, sm_ref, sl_ref, code, kb, vb, in_sem, out_sem)


def attn_body(layer, n_kv, n_steps, sp_size, ahead, len_ref, q_ref, kn_ref, vn_ref, k_hbm, v_hbm,
              ko_hbm, vo_hbm, o_ref, sm_ref, sl_ref, code, kb, vb, in_sem, out_sem):
    my_sp = lax.axis_index('sp').astype(jnp.int32)
    heads, all_rows, hd = q_ref.shape
    n_batch = all_rows // n_steps
    n_iter = n_batch // SEQS
    r8 = 2 * n_steps
    rows = heads * r8
    n_cols = kb.shape[2]
    row_kv = rows // n_kv

    def reads(i):
        slot = lax.rem(i, SLOTS)
        src = pl.ds(i * SEQS, SEQS)
        return (pltpu.make_async_copy(k_hbm.at[layer, src], kb.at[slot], in_sem.at[slot, 0]),
                pltpu.make_async_copy(v_hbm.at[layer, src], vb.at[slot], in_sem.at[slot, 1]))

    def writes(i):
        slot = lax.rem(i, SLOTS)
        dst = pl.ds(i * SEQS, SEQS)
        return (pltpu.make_async_copy(kb.at[slot], ko_hbm.at[layer, dst], out_sem.at[slot, 0]),
                pltpu.make_async_copy(vb.at[slot], vo_hbm.at[layer, dst], out_sem.at[slot, 1]))

    for i in range(min(AHEAD, n_iter)):
        for cp in reads(i):
            cp.start()

    ri = lax.broadcasted_iota(jnp.int32, (rows, n_cols), 0)
    ci = lax.broadcasted_iota(jnp.int32, (rows, n_cols), 1)
    same = (ci % n_kv) == (ri // row_kv)
    code[...] = jnp.where(same, (ci // n_kv) * sp_size + my_sp, 2**30)
    sm_ref[...] = jnp.zeros_like(sm_ref)
    sl_ref[...] = jnp.zeros_like(sl_ref)
    rcol = lax.broadcasted_iota(jnp.int32, (rows, 1), 0) % r8
    first = rcol < n_steps
    row16 = lax.broadcasted_iota(jnp.int32, (16, hd), 0)
    lane = lax.broadcasted_iota(jnp.int32, sm_ref.shape, 1)
    per = 16 // n_kv
    ahead()

    def body(i, _):
        slot_b = lax.rem(i, SLOTS)
        for cp in reads(i):
            cp.wait()
        for b in range(SEQS):
            seq = i * SEQS + b
            length = len_ref[seq]
            step = lax.rem(my_sp - lax.rem(length, sp_size) + sp_size, sp_size)
            slot = lax.div(length + step, sp_size)
            base = pl.multiple_of(lax.div(slot, per) * 16, 16)
            mine = row16 // n_kv == lax.rem(slot, per)
            new_row = seq * n_steps + step
            for buf, src in ((kb, kn_ref), (vb, vn_ref)):
                fresh = jnp.broadcast_to(src[0, pl.ds(new_row, 1), :], (16, hd))
                for j in range(1, n_kv):
                    fresh = jnp.where(row16 % n_kv == j, jnp.broadcast_to(src[j, pl.ds(new_row, 1), :], (16, hd)), fresh)
                old = buf[slot_b, b, pl.ds(base, 16), :]
                buf[slot_b, b, pl.ds(base, 16), :] = jnp.where(mine, fresh, old.astype(F32)).astype(BF16)
        for cp in writes(i):
            cp.start()
        sm, sl = sm_ref[...], sl_ref[...]
        for t in range(SEQS // 2):
            pair = i * (SEQS // 2) + t
            r0 = pl.multiple_of(pair * r8, r8)
            q = q_ref[:, pl.ds(r0, r8), :].reshape(rows, hd)
            limit = jnp.where(first, len_ref[2 * pair], len_ref[2 * pair + 1]) + rcol % n_steps
            zero = jnp.zeros_like(q)
            q2 = jnp.concatenate([jnp.where(first, q, zero), jnp.where(first, zero, q)], axis=1).astype(BF16)
            k2 = jnp.concatenate([kb[slot_b, 2 * t], kb[slot_b, 2 * t + 1]], axis=1)
            s = lax.dot_general(q2, k2, (((1,), (1,)), ((), ())), preferred_element_type=F32)
            s = jnp.where(code[...] <= limit, s * hd ** -0.5, -1e30)
            m = jnp.max(s, axis=-1, keepdims=True)
            p = jnp.exp(s - m)
            l = jnp.sum(p, axis=-1, keepdims=True)
            v2 = jnp.concatenate([vb[slot_b, 2 * t], vb[slot_b, 2 * t + 1]], axis=1)
            o = jnp.dot(p.astype(BF16), v2, preferred_element_type=F32)
            o = jnp.where(first, o[:, :hd], o[:, hd:])
            o_ref[:, pl.ds(r0, r8), :] = o.reshape(heads, r8, hd)
            sm = jnp.where(lane == pair, m, sm)
            sl = jnp.where(lane == pair, l, sl)
        sm_ref[...] = sm
        sl_ref[...] = sl

        if AHEAD < n_iter:
            @pl.when(jnp.logical_and(i + AHEAD >= SLOTS, i + AHEAD < n_iter))
            def _():
                for cp in writes(i + AHEAD - SLOTS):
                    cp.wait()

            @pl.when(i + AHEAD < n_iter)
            def _():
                for cp in reads(i + AHEAD):
                    cp.start()
        return 0

    lax.fori_loop(0, n_iter, body, 0)
    for i in range(max(0, n_iter - SLOTS), n_iter):
        for cp in writes(i):
            cp.wait()


def attn_call(layer, lengths, ins, kc, vc, prev, n_kv, n_steps, sp_size, first_pos):
    n_layers, n_batch, n_cols, hd = kc.shape
    rows = n_batch * n_steps
    V = pltpu.VMEM
    dma = pltpu.SemaphoreType.DMA
    vm = pl.BlockSpec(memory_space=V)
    hbm = pl.BlockSpec(memory_space=pl.ANY)
    smem = pl.BlockSpec(memory_space=pltpu.SMEM)
    if prev is None:
        table, u, gain, wq, wk, wv = ins
        heads, d_model = wq.shape[2] // hd, u.shape[1]
        cols = wk.shape[2]
        kernel = functools.partial(first_kernel, n_kv, n_steps, sp_size, first_pos)
        in_specs = [smem, vm, vm, vm, hbm, hbm, hbm, hbm, hbm]
        args = [lengths, *ins, kc, vc]
        aliases = {}
        more_out = [jax.ShapeDtypeStruct((rows, hd), F32)] * 2 + [jax.ShapeDtypeStruct(u.shape, BF16)]
        scratch = [
            V((heads, rows, hd), F32), V((n_kv, rows, hd), F32), V((n_kv, rows, hd), F32), V(u.shape, BF16),
            V((wq.shape[2] // cols, d_model, cols), BF16), V((d_model, cols), BF16), V((d_model, cols), BF16),
            dma((wq.shape[2] // cols + 2,)),
        ]
    else:
        heads = ins[0].shape[0]
        kernel = functools.partial(attn_kernel, layer, n_kv, n_steps, sp_size)
        in_specs = [smem, vm, vm, vm, hbm, hbm, hbm, hbm]
        args = [lengths, *ins, kc, vc, *prev]
        aliases = {6: 0, 7: 1}
        more_out = []
        scratch = []
    srows = heads * 2 * n_steps
    return pl.pallas_call(
        kernel,
        in_specs=in_specs,
        out_specs=[hbm, hbm, vm, vm, vm] + [vm] * len(more_out),
        out_shape=[
            jax.ShapeDtypeStruct(kc.shape, kc.dtype), jax.ShapeDtypeStruct(vc.shape, vc.dtype),
            jax.ShapeDtypeStruct((heads, rows, hd), F32),
            jax.ShapeDtypeStruct((srows, 128), F32), jax.ShapeDtypeStruct((srows, 128), F32),
        ] + more_out,
        scratch_shapes=scratch + [
            V((srows, n_cols), jnp.int32),
            V((SLOTS, SEQS, n_cols, hd), BF16), V((SLOTS, SEQS, n_cols, hd), BF16),
            dma((SLOTS, 2)), dma((SLOTS, 2)),
        ],
        input_output_aliases=aliases,
        compiler_params=pltpu.CompilerParams(vmem_limit_bytes=VMEM_ALL),
        name=f'attn{layer}',
    )(*args)


def block_kernel(layer, last, n_steps, o_hbm, sm_hbm, sl_hbm, u_hbm, gain_ref, wo_hbm, wg_hbm, wu_hbm, wd_hbm, *refs):
    has_next = not last
    if has_next:
        gain_a_ref, cos_ref, sin_ref, wq_hbm, wk_hbm, wv_hbm, out_ref, q_ref, k_ref, v_ref, *refs = refs
    else:
        out_ref, *refs = refs
    block_body(layer, last, n_steps, has_next, o_hbm, sm_hbm, sl_hbm, u_hbm, gain_ref, wo_hbm, wg_hbm, wu_hbm, wd_hbm,
               (gain_a_ref, cos_ref, sin_ref, wq_hbm, wk_hbm, wv_hbm) if has_next else None, out_ref,
               (q_ref, k_ref, v_ref) if has_next else None, *refs)


def block_body(layer, last, n_steps, has_next, o_hbm, sm_hbm, sl_hbm, u_hbm, gain_ref, wo_hbm, wg_hbm, wu_hbm, wd_hbm, nxt, out_ref, qkv,
                 o_ref, sm_ref, sl_ref, u_ref, in_sem, wo_v, wg_v, wu_v, wd_v, part, g1, g2, h2, act, att,
                 r_d, r_x1, r_y1, r_x2, r_y2, r_o, r_st, mo_s, mo_k, mst, r_o2, r_st2,
                 wo_sem, wg_sem, wu_sem, wd_sem, m_send, m_recv, rs_send, rs_recv, ag_send, ag_recv):
    if has_next:
        gain_a_ref, cos_ref, sin_ref, wq_hbm, wk_hbm, wv_hbm = nxt
        q_ref, k_ref, v_ref = qkv
    sp = lax.axis_index('sp')
    y = lax.axis_index('tp')
    c = lax.rem(sp, 2)
    x = lax.div(sp, 2)
    rows = u_ref.shape[0]
    d_model = u_ref.shape[1]
    hd = o_ref.shape[2]
    heads = o_ref.shape[0]
    n_pieces = d_model // PC
    f_loc = wd_v.shape[1]
    k_loc = wo_v.shape[1]
    n_f = wg_v.shape[0]
    core_dev = {'sp': 2 * x + 1 - c}
    x_dev = {'sp': 2 * (1 - x) + c}
    y_dev = {'tp': 1 - y}

    def piece(half, kind, far, sub):
        return half * 8 + kind * 4 + far * 2 + sub

    order = []
    for far_x, far_y in ((1 - x, 1 - y), (x, y)):
        for half in (1 - c, c):
            for kind, far in ((0, far_x), (1, far_y)):
                for sub in ((1 - y, y) if kind == 0 else (1 - x, x)):
                    order.append(piece(half, kind, far, sub))

    in_copies = {}
    half_rows = rows // 2
    half_of = [pl.ds(r * half_rows, half_rows) for r in range(2)]
    for n, (key, src, dst) in enumerate((
            ('m', sm_hbm, sm_ref), ('l', sl_hbm, sl_ref), (0, o_hbm.at[:, half_of[0]], o_ref.at[:, half_of[0]]),
            (1, o_hbm.at[:, half_of[1]], o_ref.at[:, half_of[1]]), ('u', u_hbm, u_ref))):
        in_copies[key] = pltpu.make_async_copy(src, dst, in_sem.at[n])
        in_copies[key].start()
    copies = {}

    def start(key, src, dst, sem):
        cp = pltpu.make_async_copy(src, dst, sem)
        cp.start()
        copies[key] = cp

    rem_row = pl.multiple_of((8 * c + 4 * x) * hd, hd)
    for i in range(n_pieces):
        start(('o', i), wo_hbm.at[layer, pl.ds(rem_row, k_loc), pl.ds(pl.multiple_of(order[i] * PC, PC), PC)],
              wo_v.at[i // 2, :, (i % 2) * PC:(i % 2 + 1) * PC], wo_sem.at[i])

    barrier = pltpu.get_barrier_semaphore()
    for dev in (core_dev, x_dev, y_dev):
        pl.semaphore_signal(barrier, inc=1, device_id=dev, device_id_type=MESH)
    pl.semaphore_wait(barrier, 3)

    def remote(src, dst, send, recv, dev):
        cp = pltpu.make_async_remote_copy(src_ref=src, dst_ref=dst, send_sem=send, recv_sem=recv, device_id=dev, device_id_type=MESH)
        cp.start()
        return cp

    hh = heads // 2
    hq = heads // 4
    sr = sm_ref.shape[0]
    away = 1 - c
    away_rows = pl.ds(pl.multiple_of(away * (sr // 2), 8), sr // 2)
    in_copies['m'].wait()
    in_copies['l'].wait()
    d_st = [remote(sm_ref.at[away_rows], r_st.at[0], m_send.at[0], m_recv.at[0], core_dev),
            remote(sl_ref.at[away_rows], r_st.at[1], m_send.at[1], m_recv.at[1], core_dev)]
    d_o = []
    for r in range(2):
        in_copies[r].wait()
        d_o.append(remote(o_ref.at[pl.ds(away * hh, hh), half_of[r]], r_o.at[:, half_of[r]], m_send.at[2 + r], m_recv.at[2 + r], core_dev))
    pending = d_st + d_o

    f_off = pl.multiple_of(sp * f_loc, PC)
    def gate_copy(i):
        col = pl.ds(pl.multiple_of(f_off + i * PC, PC), PC)
        return (pltpu.make_async_copy(wg_hbm.at[layer, :, col], wg_v.at[i], wg_sem.at[i]),
                pltpu.make_async_copy(wu_hbm.at[layer, :, col], wu_v.at[i], wu_sem.at[i]))

    for i in range(n_f):
        for cp in gate_copy(i):
            cp.start()
    for i in range(n_pieces):
        start(('d', i), wd_hbm.at[layer, pl.ds(f_off, f_loc), pl.ds(pl.multiple_of(order[i] * PC, PC), PC)],
              wd_v.at[i // 2, :, (i % 2) * PC:(i % 2 + 1) * PC], wd_sem.at[i])

    def merge_into(r, dst, st_dst, src_o, m1, l1, src_o2, m2, l2, n_heads):
        mx = jnp.maximum(m1, m2)
        f1 = jnp.exp(m1 - mx)
        f2 = jnp.exp(m2 - mx)
        ln = l1 * f1 + l2 * f2
        st_dst(mx, ln)
        for h in range(n_heads):
            for t in range(r * half_rows // 8, (r + 1) * half_rows // 8):
                a = jnp.broadcast_to(f1[8 * h:8 * h + 8, t:t + 1], (8, hd))
                b = jnp.broadcast_to(f2[8 * h:8 * h + 8, t:t + 1], (8, hd))
                dst(h, t, src_o(h, t) * a + src_o2(h, t) * b, ln)

    def core_merge(r, q4, dst_o, slot):
        lo = pl.multiple_of(c * (sr // 2) + q4 * (sr // 4), 8)
        lr = pl.multiple_of(q4 * (sr // 4), 8)
        n = sr // 4

        def st_dst(mx, ln):
            if r == 0:
                mst[slot, 0] = mx
                mst[slot, 1] = ln

        def dst(h, t, val, ln):
            dst_o[h, 8 * t:8 * t + 8, :] = val

        merge_into(r, dst, st_dst,
                   lambda h, t: o_ref[c * hh + q4 * hq + h, 8 * t:8 * t + 8, :], sm_ref[pl.ds(lo, n)], sl_ref[pl.ds(lo, n)],
                   lambda h, t: r_o[q4 * hq + h, 8 * t:8 * t + 8, :], r_st[0, pl.ds(lr, n)], r_st[1, pl.ds(lr, n)], hq)

    x_st = []

    def merge_chain(r):
        if r == 0:
            for cp in d_st:
                cp.wait_recv()
        d_o[r].wait_recv()
        core_merge(r, 1 - x, mo_s, 0)
        if r == 0:
            x_st.append(remote(mst.at[0], r_st2, m_send.at[4], m_recv.at[4], x_dev))
            pending.append(x_st[0])
        x_o = remote(mo_s.at[:, half_of[r]], r_o2.at[:, half_of[r]], m_send.at[5 + r], m_recv.at[5 + r], x_dev)
        pending.append(x_o)
        core_merge(r, x, mo_k, 1)
        yield
        if r == 0:
            x_st[0].wait_recv()
        x_o.wait_recv()

        def fin(h, t, val, ln):
            den = jnp.broadcast_to(ln[8 * h:8 * h + 8, t:t + 1], (8, hd))
            mo_k[h, 8 * t:8 * t + 8, :] = val / den

        merge_into(r, fin, lambda mx, ln: None,
                   lambda h, t: mo_k[h, 8 * t:8 * t + 8, :], mst[1, 0], mst[1, 1],
                   lambda h, t: r_o2[h, 8 * t:8 * t + 8, :], r_st2[0], r_st2[1], hq)
        for h in range(hq):
            att[half_of[r], h * hd:(h + 1) * hd] = mo_k[h, half_of[r]].astype(BF16)

    def rs(r, n, src, dst, dev):
        cp = remote(src, dst, rs_send.at[10 * r + n], rs_recv.at[10 * r + n], dev)
        pending.append(cp)
        return cp

    def sum_front(halves, product):
        r0 = halves[0]
        R = pl.ds(r0 * half_rows, len(halves) * half_rows)
        link = {r: [None] * 4 for r in halves}

        def core_part(first, at):
            out = []
            for k in range(2):
                i = first + 2 * k
                val = product(i // 2, R, r0 == 0)
                part[i, R] = val[:, :PC]
                part[i + 1, R] = val[:, PC:]
                out.append(rs(r0, at // 2 + k, part.at[pl.ds(i, 2), R], r_d.at[pl.ds(at + 2 * k, 2), R], core_dev))
            return out

        def own_part(first, at, k, d_in):
            i = first + 2 * k
            val = product(i // 2, R, r0 == 0)
            d_in[k].wait_recv()
            part[i, R] = val[:, :PC] + r_d[at + 2 * k, R]
            part[i + 1, R] = val[:, PC:] + r_d[at + 2 * k + 1, R]

        d_in = core_part(0, 0)
        for k, (buf, dev) in enumerate(((r_x1, x_dev), (r_y1, y_dev))):
            own_part(4, 0, k, d_in)
            for r in halves:
                for j in range(2):
                    link[r][2 * k + j] = rs(r, 4 + 2 * k + j, part.at[4 + 2 * k + j, half_of[r]], buf.at[j, half_of[r]], dev)
        d_in = core_part(8, 4)
        for k in range(2):
            own_part(12, 4, k, d_in)
        return link

    def sum_back(r, link, resid, g):
        R = half_of[r]

        def ag(n, p, dev):
            cp = remote(g.at[p, R], g.at[p, R], ag_send.at[14 * r + n], ag_recv.at[14 * r + n], dev)
            pending.append(cp)
            return cp

        link[0].wait_recv()
        part[12, R] = part[12, R] + r_x1[0, R]
        a2 = rs(r, 8, part.at[12, R], r_y2.at[R], y_dev)
        link[2].wait_recv()
        part[14, R] = part[14, R] + r_y1[0, R]
        b2 = rs(r, 9, part.at[14, R], r_x2.at[R], x_dev)
        link[1].wait_recv()
        part[13, R] = part[13, R] + r_x1[1, R]
        link[3].wait_recv()
        part[15, R] = part[15, R] + r_y1[1, R]
        yield
        pa = piece(c, 0, x, y)
        pb = piece(c, 1, y, x)
        a2.wait_recv()
        g[pa, R] = (resid(pa, R) + (part[13, R] + r_y2[R])).astype(BF16).astype(F32)
        ya = ag(0, pa, y_dev)
        b2.wait_recv()
        g[pb, R] = (resid(pb, R) + (part[15, R] + r_x2[R])).astype(BF16).astype(F32)
        xb = ag(3, pb, x_dev)
        xa = ag(1, pa, x_dev)
        yb = ag(4, pb, y_dev)
        last_in = [ag(2, pa, core_dev), ag(5, pb, core_dev)]
        yield
        ya.wait_recv()
        p = piece(c, 0, x, 1 - y)
        xf = ag(6, p, x_dev)
        last_in.append(ag(7, p, core_dev))
        xb.wait_recv()
        p = piece(c, 1, y, 1 - x)
        yf = ag(8, p, y_dev)
        last_in.append(ag(9, p, core_dev))
        yield
        xa.wait_recv()
        last_in.append(ag(10, piece(c, 0, 1 - x, y), core_dev))
        yb.wait_recv()
        last_in.append(ag(11, piece(c, 1, 1 - y, x), core_dev))
        xf.wait_recv()
        last_in.append(ag(12, piece(c, 0, 1 - x, 1 - y), core_dev))
        yf.wait_recv()
        last_in.append(ag(13, piece(c, 1, 1 - y, 1 - x), core_dev))
        yield
        for cp in last_in:
            cp.wait_recv()

    def interleave(chains):
        chains = list(chains)
        while chains:
            for ch in list(chains):
                if next(ch, 'end') == 'end':
                    chains.remove(ch)
        for cp in pending:
            cp.wait_send()
        pending.clear()

    def out_product(k, R, fetch):
        if fetch:
            copies[('o', 2 * k)].wait()
            copies[('o', 2 * k + 1)].wait()
        return jnp.dot(att[R], wo_v[k], preferred_element_type=F32)

    def u_resid(p, R):
        return u_ref[R, pl.ds(pl.multiple_of(p * PC, PC), PC)].astype(F32)

    def first_part(r):
        yield from merge_chain(r)
        link = sum_front([r], out_product)
        yield
        if r == 0:
            in_copies['u'].wait()
        yield from sum_back(r, link[r], u_resid, g1)

    interleave(first_part(r) for r in range(2))

    def norm(g, gains, row):
        sq = jnp.zeros((rows, PC), F32)
        for i in range(n_pieces):
            sq = sq + g[i] * g[i]
        inv = lax.rsqrt(jnp.sum(sq, axis=-1, keepdims=True) * (1.0 / d_model) + EPS)
        for i in range(n_pieces):
            cols = slice(i * PC, (i + 1) * PC)
            h2[:, cols] = (g[i] * inv * gains[row:row + 1, cols].astype(F32)).astype(BF16)

    norm(g1, gain_ref, layer)

    def gate_up(i, _):
        cg, cu = gate_copy(i)
        cg.wait()
        ga = jnp.dot(h2[...], wg_v[i], preferred_element_type=F32)
        cu.wait()
        up = jnp.dot(h2[...], wu_v[i], preferred_element_type=F32)
        act[:, pl.ds(pl.multiple_of(i * PC, PC), PC)] = (ga * jax.nn.sigmoid(ga) * up).astype(BF16)
        return 0

    lax.fori_loop(0, n_f, gate_up, 0)

    n_q = q_ref.shape[0] * hd // (2 * PC) if has_next else 0

    def next_copy(j):
        out = []
        for t, (buf, sem) in enumerate(((wg_v, wg_sem), (wu_v, wu_sem))):
            if isinstance(j, int) and j >= n_q:
                src = (wk_hbm, wv_hbm)[j - n_q].at[layer + 1, :, t * PC:(t + 1) * PC]
            else:
                src = wq_hbm.at[layer + 1, :, pl.ds(pl.multiple_of((2 * j + t) * PC, PC), PC)]
            out.append(pltpu.make_async_copy(src, buf.at[j], sem.at[j]))
        return out

    if has_next:
        for j in range(n_q + 2):
            for cp in next_copy(j):
                cp.start()

    def down_product(k, R, fetch):
        copies[('d', 2 * k)].wait()
        copies[('d', 2 * k + 1)].wait()
        return jnp.dot(act[...], wd_v[k], preferred_element_type=F32)

    links = sum_front([0, 1], down_product)
    interleave(sum_back(r, links[r], lambda p, R: g1[p, R], g2) for r in range(2))
    back = permutation(rows, n_steps, False) if last else None
    for i in range(n_pieces):
        val = g2[i].astype(BF16)
        if last:
            val = jnp.dot(back, val, preferred_element_type=F32).astype(BF16)
        out_ref[:, i * PC:(i + 1) * PC] = val

    if has_next:
        norm(g2, gain_a_ref, layer + 1)
        cos_a, sin_a = cos_ref[...], sin_ref[...]

        def rot(z):
            return (z * cos_a + pltpu.roll(z, hd // 2, 1) * sin_a).astype(BF16).astype(F32)

        def heads_of(j, store):
            for t, (buf, cp) in enumerate(zip((wg_v, wu_v), next_copy(j))):
                cp.wait()
                val = jnp.dot(h2[...], buf[j], preferred_element_type=F32)
                for e in range(PC // hd):
                    store(t * (PC // hd) + e, val[:, e * hd:(e + 1) * hd])

        def q_pair(j, _):
            def store(e, val):
                q_ref[2 * (PC // hd) * j + e] = rot(val)
            heads_of(j, store)
            return 0

        def store_k(e, val):
            k_ref[e] = rot(val)

        def store_v(e, val):
            v_ref[e] = val.astype(BF16).astype(F32)

        lax.fori_loop(0, n_q, q_pair, 0)
        heads_of(n_q, store_k)
        heads_of(n_q + 1, store_v)


def block_call(layer, last, n_steps, o, sm, sl, u, gain, wo, wg, wu, wd, sp_size, nxt):
    rows, d_model = u.shape
    heads, _, hd = o.shape
    n_p = d_model // PC
    k_loc = wo.shape[1] // sp_size
    f_loc = wd.shape[1] // sp_size
    n_f = f_loc // PC
    sr = sm.shape[0]
    V = pltpu.VMEM
    dma = pltpu.SemaphoreType.DMA
    vm = pl.BlockSpec(memory_space=pltpu.VMEM)
    hbm = pl.BlockSpec(memory_space=pl.ANY)
    return pl.pallas_call(
        functools.partial(block_kernel, layer, last, n_steps),
        out_shape=[jax.ShapeDtypeStruct((rows, d_model), BF16)] + ([] if last else [
            jax.ShapeDtypeStruct((heads, rows, hd), F32),
            jax.ShapeDtypeStruct((nxt[4].shape[2] // hd, rows, hd), F32),
            jax.ShapeDtypeStruct((nxt[4].shape[2] // hd, rows, hd), F32)]),
        in_specs=[hbm] * 4 + [vm] + [hbm] * 4 + ([] if last else [vm] * 3 + [hbm] * 3),
        out_specs=[vm] * (1 if last else 4),
        scratch_shapes=[
            V(o.shape, F32), V(sm.shape, F32), V(sl.shape, F32), V(u.shape, BF16), dma((5,)),
            V((n_p // 2, k_loc, 2 * PC), BF16), V((n_f, d_model, PC), BF16), V((n_f, d_model, PC), BF16), V((n_p // 2, f_loc, 2 * PC), BF16),
            V((n_p, rows, PC), F32), V((n_p, rows, PC), F32), V((n_p, rows, PC), F32),
            V((rows, d_model), BF16), V((rows, f_loc), BF16), V((rows, k_loc), BF16),
            V((n_p // 2, rows, PC), F32), V((2, rows, PC), F32), V((2, rows, PC), F32), V((rows, PC), F32), V((rows, PC), F32),
            V((heads // 2, rows, hd), F32), V((2, sr // 2, 128), F32),
            V((heads // 4, rows, hd), F32), V((heads // 4, rows, hd), F32), V((2, 2, sr // 4, 128), F32),
            V((heads // 4, rows, hd), F32), V((2, sr // 4, 128), F32),
            dma((n_p,)), dma((n_f,)), dma((n_f,)), dma((n_p,)),
            dma((7,)), dma((7,)), dma((20,)), dma((20,)), dma((28,)), dma((28,)),
        ],
        compiler_params=pltpu.CompilerParams(collective_id=layer, has_side_effects=True, vmem_limit_bytes=VMEM_ALL),
        name=f'block{layer}',
    )(o, sm, sl, u, gain, wo, wg, wu, wd, *nxt)


def solution(mesh):
    sp_size = mesh.shape['sp']

    def local_fn(tok_emb, lengths, key_cache, val_cache, gain_attn, gain_mlp, w_query, w_key, w_value, w_out, w_gate, w_up, w_down):
        n_steps, n_batch, d_model = tok_emb.shape
        n_layers, _, loc_len, kv_loc, hd = key_cache.shape
        rows = n_steps * n_batch
        first_pos = loc_len * sp_size // 2
        table = jnp.asarray(rope_table(first_pos, first_pos, hd))
        u = tok_emb.reshape(rows, d_model)
        kc = key_cache.reshape(n_layers, n_batch, loc_len * kv_loc, hd)
        vc = val_cache.reshape(n_layers, n_batch, loc_len * kv_loc, hd)
        prev = None
        for layer in range(n_layers):
            last = layer == n_layers - 1
            ins = (table, u, gain_attn, w_query, w_key, w_value) if layer == 0 else (q, k, v)
            nk, nv, o, sm, sl, *more = attn_call(layer, lengths, ins, kc, vc, prev, kv_loc, n_steps, sp_size, first_pos)
            if layer == 0:
                cos_a, sin_a, u = more
            prev = (nk, nv)
            nxt = () if last else (gain_attn, cos_a, sin_a, w_query, w_key, w_value)
            outs = block_call(layer, last, n_steps, o, sm, sl, u, gain_mlp, w_out, w_gate, w_up, w_down, sp_size, nxt)
            u = outs[0]
            if not last:
                q, k, v = outs[1:]
        return u.reshape(n_steps, n_batch, d_model), prev[0].reshape(key_cache.shape), prev[1].reshape(val_cache.shape)

    cache_spec = P(None, 'dp', 'sp', 'tp', None)
    col_spec = P(None, None, 'tp')
    row_spec = P(None, 'tp', None)
    emb_spec = P(None, 'dp', None)
    return jax.shard_map(local_fn, mesh=mesh, in_specs=(emb_spec, P('dp'), cache_spec, cache_spec, P(), P(), col_spec, col_spec, col_spec, row_spec, col_spec, col_spec, row_spec), out_specs=(emb_spec, cache_spec, cache_spec), check_vma=False)
```
